256 devices in a mesh: gx: 4 (over y), gy: 8 (over x, core), gz: 8 (over z).
Axes of the slice: x: 4, y: 4, z: 8, core: 2. Of those that a mesh axis runs over, the one named last changes fastest.
Arguments:
- measures: float32 [524288, 256], P(('gx', 'gy', 'gz')), may hold values from -6 to 6
- group_index: int32 [524288], P(('gx', 'gy', 'gz')), may hold values from 0 to 511, as said below
- distinct_keys: int32 [256, 512], P(('gx', 'gy', 'gz')), may hold values from 256 to 524543, as said below
- group_counts: int32 [256], P(('gx', 'gy', 'gz')), may hold values from 128 to 512, as said below
Outputs:
- group_sums: float32 [131072, 256], P(('gx', 'gy', 'gz'))
- group_rows: int32 [131072], P(('gx', 'gy', 'gz'))
- group_keys: int32 [131072], P(('gx', 'gy', 'gz'))
- group_total: int32 [], replicated
The draws below stay inside these ranges and needn't reach their ends.
Inputs may be any that keep to these rules, and one draw needn't show every extreme that they name: `group_counts`: every device has between 128 and 512 groups, and some device has exactly 512. `group_index`: each row's index lies below its device's group count, and every group of a device has at least one row. `distinct_keys`: each device's keys rise strictly; all keys of device d equal d modulo 256, so no key lives on two devices; entries at and past the device's count are unused.
All inputs are finite; a program needn't handle non-finite values.
Results may differ from the reference program's by a relative error of at most 0.0003.
Values sent between devices are 32-bit elements; how exact they have to be, the bound alone decides.
A program may use at most 64 MiB of HBM per device.

```python
import jax
import jax.numpy as jnp
from jax import lax

ROW_DEV = 2048
M = 256
GMAX = 512
ROWS = 524288
DEVICES = 256


def shared_counts(key):
    counts = jax.random.randint(jax.random.fold_in(key, 7), (DEVICES,), GMAX // 4, GMAX + 1)
    fullest = jax.random.randint(jax.random.fold_in(key, 8), (), 0, DEVICES)
    return counts.at[fullest].set(GMAX).astype(jnp.int32)


def draw_group_counts(key, part):
    return shared_counts(key)


def one_device(key, count):
    places = jnp.arange(ROW_DEV, dtype=jnp.int32)
    upper = jnp.minimum(jax.random.randint(jax.random.fold_in(key, 1), (ROW_DEV,), 1, GMAX + 1), count)
    picked = jax.random.randint(jax.random.fold_in(key, 2), (ROW_DEV,), 0, upper)
    picked = jnp.where(places < count, places, picked % count)
    order = jax.random.permutation(jax.random.fold_in(key, 3), ROW_DEV)
    return picked[order].astype(jnp.int32)


def draw_group_index(key, part):
    counts = shared_counts(key)
    device_keys = jax.vmap(lambda d: jax.random.fold_in(jax.random.fold_in(key, 11), d))(jnp.arange(DEVICES))
    return jax.vmap(one_device)(device_keys, counts).reshape(-1)


def draw_distinct_keys(key, part):
    steps = jax.random.randint(jax.random.fold_in(key, 21), (DEVICES, GMAX), 1, 5)
    steps = steps.at[0, 0].set(1)
    rising = jnp.cumsum(steps, axis=1)
    rising = rising.at[:, GMAX - 1].set(4 * GMAX)
    owner = jnp.arange(DEVICES, dtype=jnp.int32)[:, None]
    return (owner + DEVICES * rising).astype(jnp.int32)


def shard_levels(key, extent, pieces, least, top_value):
    loudness = 1.0
    for dim, blocks in pieces:
        draws = jax.random.uniform(jax.random.fold_in(jax.random.fold_in(key, 6), dim), (blocks,), jnp.float32, least / len(pieces), top_value / len(pieces))
        loudness = loudness * jnp.repeat(jnp.exp(draws), extent[dim] // blocks).reshape((-1,) + (1,) * (len(extent) - 1 - dim))
    return loudness


def gaussian(key, dims, width, limit, split=(), held_as=jnp.bfloat16):
    drawn = width * jax.random.normal(key, dims, jnp.float32)
    if split:
        drawn = drawn * shard_levels(key, dims, split, -0.22, 0.18)
    return jnp.clip(drawn, -limit, limit).astype(held_as)


def setup_inputs(seed: int = 0) -> dict:
    arg_keys = jax.random.split(jax.random.key(seed), 5)
    measures = gaussian(arg_keys[0], (ROWS, M), 1.0, 6.0, ((0, 256),), jnp.float32)
    group_index = draw_group_index(jax.random.fold_in(arg_keys[4], 71), 0)
    distinct_keys = draw_distinct_keys(jax.random.fold_in(arg_keys[4], 71), 0)
    group_counts = draw_group_counts(jax.random.fold_in(arg_keys[4], 71), 0)
    return dict(measures=measures, group_index=group_index, distinct_keys=distinct_keys, group_counts=group_counts)


def local_groups(pair):
    values, index = pair
    sums = jax.ops.segment_sum(values, index, num_segments=GMAX)
    rows = jax.ops.segment_sum(jnp.ones_like(index), index, num_segments=GMAX)
    return sums, rows


def reference(measures, group_index, distinct_keys, group_counts):
    offsets = jnp.cumsum(group_counts) - group_counts
    group_total = jnp.sum(group_counts).astype(jnp.int32)
    values = measures.reshape(DEVICES, ROW_DEV, M)
    index = group_index.reshape(DEVICES, ROW_DEV)
    sums, rows = lax.map(local_groups, (values, index))
    local = jnp.arange(GMAX, dtype=jnp.int32)
    dense = offsets[:, None] + local[None, :]
    live = local[None, :] < group_counts[:, None]
    where_to = (dense % DEVICES) * GMAX + dense // DEVICES
    where_to = jnp.where(live, where_to, DEVICES * GMAX).astype(jnp.int32).reshape(-1)
    group_sums = jnp.zeros((DEVICES * GMAX, M), jnp.float32).at[where_to].set(sums.reshape(-1, M), mode="drop")
    group_rows = jnp.zeros((DEVICES * GMAX,), jnp.int32).at[where_to].set(rows.reshape(-1).astype(jnp.int32), mode="drop")
    group_keys = jnp.full((DEVICES * GMAX,), -1, jnp.int32).at[where_to].set(distinct_keys.reshape(-1), mode="drop")
    return group_sums, group_rows, group_keys, group_total
```

```python
import functools

import jax
import jax.numpy as jnp
from jax import lax
from jax.experimental import pallas as pl
from jax.experimental.pallas import tpu as pltpu
from jax.sharding import PartitionSpec as P

AXES = ("gx", "gy", "gz")
MESH = pl.DeviceIdType.MESH
F32, BF16, I32 = jnp.float32, jnp.bfloat16, jnp.int32
CHUNKS = 4


def split2(v):
    hi = v.astype(BF16)
    lo = (v - hi.astype(F32)).astype(BF16)
    return hi, lo


def split3(v):
    hi = v.astype(BF16)
    rest = v - hi.astype(F32)
    mid = rest.astype(BF16)
    lo = (rest - mid.astype(F32)).astype(BF16)
    return hi, mid, lo


def dot(a, b):
    return jnp.dot(a, b, preferred_element_type=F32)


def kernel(
    sizes,
    measures, index, keys, count,
    out_sums, out_rows, out_keys, out_total,
    values, acc, tally, doubled, fields, outgoing, arrived, fsend, frecv, frelay, farrived,
    crow, cline, crelay, call,
    load_sems, cz_send, cz_recv, cp_send, cp_recv, fp_send, fp_recv, fz_send, fz_recv, b_send, b_recv,
):
    nx, ny, nz = sizes
    plane, devices = nx * ny, nx * ny * nz
    rows = measures.shape[0]
    step = rows // CHUNKS
    span = 2 * devices
    x, y, z = (lax.axis_index(a) for a in AXES)
    q = x * ny + y
    me = q * nz + z

    def in_line(k):
        return (z + k) % nz

    def in_plane(k):
        return (x + k // ny) % nx, (y + k % ny) % ny

    loads = [
        pltpu.make_async_copy(
            measures.at[pl.ds(c * step, step)], values.at[pl.ds(c * step, step)], load_sems.at[c]
        )
        for c in range(CHUNKS)
    ]
    for load in loads:
        load.start()

    barrier = pltpu.get_barrier_semaphore()
    for k in range(1, nz):
        pl.semaphore_signal(barrier, inc=1, device_id=(x, y, in_line(k)), device_id_type=MESH)

    @pl.loop(1, plane)
    def _(k):
        px, py = in_plane(k)
        pl.semaphore_signal(barrier, inc=1, device_id=(px, py, z), device_id_type=MESH)

    lane = lax.broadcasted_iota(I32, (1, 128), 1)
    mine = jnp.where(lane == me % 128, count[0], 0)
    crow[0] = mine
    cline[z] = mine

    labels = lax.broadcasted_iota(I32, (span, step), 0)
    ones = jnp.ones((step, 128), BF16)

    def accumulate(c):
        loads[c].wait()
        hits = jnp.where(labels == index[0:1, c * step : (c + 1) * step], 1.0, 0.0).astype(BF16)
        hi, lo = split2(values[pl.ds(c * step, step)])
        part = dot(hits, hi) + dot(hits, lo)
        seen = dot(hits, ones)
        if c == 0:
            acc[...] = part
            tally[...] = seen
        else:
            acc[...] += part
            tally[...] += seen

    accumulate(0)
    accumulate(1)
    pl.semaphore_wait(barrier, nz - 1 + plane - 1)

    for k in range(1, nz):
        pltpu.make_async_remote_copy(
            crow.at[0], cline.at[z], cz_send, cz_recv, device_id=(x, y, in_line(k)), device_id_type=MESH
        ).start()
    accumulate(2)
    accumulate(3)

    def drain(ref, n, sem):
        pltpu.make_async_copy(ref.at[pl.ds(0, n)], ref.at[pl.ds(0, n)], sem).wait()

    drain(cline, nz - 1, cz_recv)
    relayed = cline[0]
    for k in range(1, nz):
        relayed = relayed + cline[k]
    crelay[0] = relayed
    call[q] = relayed

    @pl.loop(1, plane)
    def _(k):
        px, py = in_plane(k)
        pltpu.make_async_remote_copy(
            crelay.at[0], call.at[q], cp_send, cp_recv, device_id=(px, py, z), device_id_type=MESH
        ).start()

    for level in range(2):
        for half in range(2):
            part = acc[pl.ds(level * devices, devices), pl.ds(half * 128, 128)]
            doubled[pl.ds(0, devices), 2 * level + half, :] = part
            doubled[pl.ds(devices, devices), 2 * level + half, :] = part
    flane = lax.broadcasted_iota(I32, (devices, 128), 1)
    tall_keys = jnp.broadcast_to(keys[...].astype(F32) + 1.0, (128, span)).T
    field = jnp.zeros((devices, 128), F32)
    for level in range(2):
        held = pl.ds(level * devices, devices)
        field = jnp.where(flane == level * 32 + q, tally[held, :], field)
        field = jnp.where(
            flane == 64 + level * 32 + q, tall_keys[level * devices : (level + 1) * devices], field
        )
    fields[pl.ds(0, devices), :] = field
    fields[pl.ds(devices, devices), :] = field

    drain(call, plane - 1, cp_recv)
    low = jnp.sum(call[pl.ds(0, plane // 2)], axis=0)
    high = jnp.sum(call[pl.ds(plane // 2, plane // 2)], axis=0)
    counts = jnp.concatenate([low, high], axis=1)
    lanes = lax.broadcasted_iota(I32, (1, devices), 1)
    offset = jnp.sum(jnp.where(lanes < me, counts, 0))
    start = devices - offset % devices
    fsend[...] = fields[pl.ds(start, devices), :].reshape(plane, nz, 128)

    @pl.loop(1, plane)
    def _(k):
        px, py = in_plane(k)
        pltpu.make_async_remote_copy(
            fsend.at[px * ny + py], frecv.at[q], fp_send, fp_recv, device_id=(px, py, z), device_id_type=MESH
        ).start()

    outgoing[...] = doubled[pl.ds(start, devices)]

    def send_block(k):
        i = k % nz
        dz = nz // 2 + jnp.where(i % 2 == 1, -((i + 1) // 2), i // 2)
        tz = (z + jnp.where(i == nz - 1, 0, dz)) % nz
        px, py = in_plane(plane - 1 - k // nz)
        target = (px * ny + py) * nz + tz
        pltpu.make_async_remote_copy(
            outgoing.at[target], arrived.at[me], b_send, b_recv, device_id=(px, py, tz), device_id_type=MESH
        ).start()

    pl.loop(0, devices // 2)(send_block)

    frecv[q] = fsend[q]
    drain(frecv, plane - 1, fp_recv)
    gathered = jnp.sum(frecv[...], axis=0)
    for k in range(nz):
        frelay[k] = gathered[k : k + 1]
    farrived[z] = frelay[z]
    for k in range(1, nz):
        pltpu.make_async_remote_copy(
            frelay.at[in_line(k)], farrived.at[z], fz_send, fz_recv, device_id=(x, y, in_line(k)), device_id_type=MESH
        ).start()

    pl.loop(devices // 2, devices - 1)(send_block)
    arrived[me] = outgoing[me]

    before = lax.broadcasted_iota(I32, (devices, devices), 0) < lax.broadcasted_iota(I32, (devices, devices), 1)
    before = jnp.where(before, 1.0, 0.0).astype(BF16)
    tops = jnp.broadcast_to((counts // 8).astype(F32).astype(BF16), (8, devices))
    rests = jnp.broadcast_to((counts % 8).astype(F32).astype(BF16), (8, devices))
    offsets = (8.0 * dot(tops, before) + dot(rests, before))[0:1].astype(I32)
    out_total[...] = jnp.sum(counts).reshape(1, 1)
    places = []
    for level in range(2):
        position = level * devices + (me - offsets) % devices
        place = (offsets + position) // devices
        places.append(jnp.where(position < counts, place, -1))
    place = jnp.concatenate(places, axis=1)
    picks = jnp.where(lax.broadcasted_iota(I32, (span, span), 0) == place, 1.0, 0.0).astype(BF16)

    drain(farrived, nz - 1, fz_recv)
    got = jnp.concatenate([farrived[k] for k in range(nz)], axis=0)
    wide = jnp.broadcast_to(got[None], (plane, nz, 128)).reshape(devices, 128)
    sender = lax.broadcasted_iota(I32, (devices, 128), 0) // nz
    fit = flane % 32 == sender
    in_level = (flane // 32) % 2
    chosen = jnp.concatenate(
        [jnp.where(fit & (in_level == level), wide, 0.0) for level in range(2)], axis=0
    )
    hi, mid, lo = split3(chosen)
    found = ((dot(picks, hi) + dot(picks, mid)) + dot(picks, lo)).T
    out_rows[...] = jnp.sum(found[0:64], axis=0, keepdims=True).astype(I32)
    out_keys[...] = jnp.sum(found[64:128], axis=0, keepdims=True).astype(I32) - 1

    drain(arrived, devices - 1, b_recv)
    parts = []
    for level in range(2):
        parts.append(
            jnp.concatenate([arrived[:, 2 * level + half, :] for half in range(2)], axis=1)
        )
    hi, lo = split2(jnp.concatenate(parts, axis=0))
    out_sums[...] = dot(picks, hi) + dot(picks, lo)

    drain(cline, nz - 1, cz_send)
    drain(call, plane - 1, cp_send)
    drain(fsend, plane - 1, fp_send)
    drain(farrived, nz - 1, fz_send)
    drain(outgoing, devices - 1, b_send)


def solution(mesh):
    sizes = tuple(mesh.shape[a] for a in AXES)
    nx, ny, nz = sizes
    plane, devices = nx * ny, nx * ny * nz
    vmem = pl.BlockSpec(memory_space=pltpu.VMEM)

    def shards(measures, group_index, distinct_keys, group_counts):
        rows, width = measures.shape
        span = distinct_keys.shape[1]
        sums, tallies, keys, total = pl.pallas_call(
            functools.partial(kernel, sizes),
            out_shape=(
                jax.ShapeDtypeStruct((span, width), F32),
                jax.ShapeDtypeStruct((1, span), I32),
                jax.ShapeDtypeStruct((1, span), I32),
                jax.ShapeDtypeStruct((1, 1), I32),
            ),
            in_specs=[
                pl.BlockSpec(memory_space=pl.ANY),
                vmem,
                vmem,
                pl.BlockSpec(memory_space=pltpu.SMEM),
            ],
            out_specs=(vmem, vmem, vmem, vmem),
            scratch_shapes=[
                pltpu.VMEM((rows, width), F32),
                pltpu.VMEM((span, width), F32),
                pltpu.VMEM((span, 128), F32),
                pltpu.VMEM((span, 4, 128), F32),
                pltpu.VMEM((span, 128), F32),
                pltpu.VMEM((devices, 4, 128), F32),
                pltpu.VMEM((devices, 4, 128), F32),
                pltpu.VMEM((plane, nz, 128), F32),
                pltpu.VMEM((plane, nz, 128), F32),
                pltpu.VMEM((nz, 1, 128), F32),
                pltpu.VMEM((nz, 1, 128), F32),
                pltpu.VMEM((1, 1, 128), I32),
                pltpu.VMEM((nz, 1, 128), I32),
                pltpu.VMEM((1, 1, 128), I32),
                pltpu.VMEM((plane, 1, 128), I32),
                pltpu.SemaphoreType.DMA((CHUNKS,)),
            ]
            + [pltpu.SemaphoreType.DMA(())] * 10,
            compiler_params=pltpu.CompilerParams(collective_id=0, has_side_effects=True),
            name="groups",
        )(measures, group_index.reshape(1, rows), distinct_keys, group_counts)
        return sums, tallies.reshape(span), keys.reshape(span), total.reshape(())

    return jax.shard_map(
        shards,
        mesh=mesh,
        in_specs=(P(AXES, None), P(AXES), P(AXES, None), P(AXES)),
        out_specs=(P(AXES, None), P(AXES), P(AXES), P()),
        check_vma=False,
    )
```

```python
import functools

import jax
import jax.numpy as jnp
from jax import lax
from jax.experimental import pallas as pl
from jax.experimental.pallas import tpu as pltpu
from jax.sharding import PartitionSpec as P

AXES = ("gx", "gy", "gz")
MESH = pl.DeviceIdType.MESH
F32, BF16, I32 = jnp.float32, jnp.bfloat16, jnp.int32
CHUNKS = 4
FIRST = 20


def split2(v):
    hi = v.astype(BF16)
    lo = (v - hi.astype(F32)).astype(BF16)
    return hi, lo


def split3(v):
    hi = v.astype(BF16)
    rest = v - hi.astype(F32)
    mid = rest.astype(BF16)
    lo = (rest - mid.astype(F32)).astype(BF16)
    return hi, mid, lo


def dot(a, b):
    return jnp.dot(a, b, preferred_element_type=F32)


def kernel(
    sizes,
    measures, index_in, keys_in,
    arrived, small,
    values, index, keys, acc, tally, doubled, fields, outgoing, fsend, frecv, frelay, farrived,
    crow, cline, crelay, call,
    load_sems, own_sem, cz_send, cz_recv, cp_send, cp_recv, fp_send, fp_recv, fz_send, fz_recv, b_send, b_recv,
):
    nx, ny, nz = sizes
    plane, devices = nx * ny, nx * ny * nz
    rows = measures.shape[0]
    step = rows // CHUNKS
    span = 2 * devices
    x, y, z = (lax.axis_index(a) for a in AXES)
    q = x * ny + y
    me = q * nz + z

    def outward(n):
        return sorted(range(n), key=lambda k: -min(k, n - k))

    def moved(base, k, n):
        return lax.rem(base + k, n) if k else base

    lines = [(k, moved(z, k, nz)) for k in outward(nz) if k]
    across = sorted(
        ((i, j) for i in range(nx) for j in range(ny) if i or j),
        key=lambda t: -(min(t[0], nx - t[0]) + min(t[1], ny - t[1]) / 2),
    )
    xs = [moved(x, k, nx) for k in range(nx)]
    ys = [moved(y, k, ny) for k in range(ny)]
    peers = [(xs[i], ys[j]) for i, j in across]

    loads = [
        pltpu.make_async_copy(
            measures.at[pl.ds(c * step, step)], values.at[pl.ds(c * step, step)], load_sems.at[c]
        )
        for c in range(CHUNKS)
    ]
    inputs = [
        pltpu.make_async_copy(src, dst, load_sems.at[CHUNKS + i])
        for i, (src, dst) in enumerate(((index_in, index), (keys_in, keys)))
    ]
    for load in inputs + loads:
        load.start()

    barrier = pltpu.get_barrier_semaphore()
    for _, tz in lines:
        pl.semaphore_signal(barrier, inc=1, device_id=(x, y, tz), device_id_type=MESH)
    for px, py in peers:
        pl.semaphore_signal(barrier, inc=1, device_id=(px, py, z), device_id_type=MESH)

    for load in inputs:
        load.wait()
    count = jnp.max(index[...], axis=1, keepdims=True) + 1
    lane = lax.broadcasted_iota(I32, (1, 128), 1)
    mine = jnp.where(lane == me % 128, count, 0)
    crow[0] = mine
    cline[z] = mine

    labels = lax.broadcasted_iota(I32, (span, step), 0)
    ones = jnp.ones((step, 128), BF16)

    def accumulate(c):
        loads[c].wait()
        hits = jnp.where(labels == index[0:1, c * step : (c + 1) * step], 1.0, 0.0).astype(BF16)
        hi, lo = split2(values[pl.ds(c * step, step)])
        part = dot(hits, hi) + dot(hits, lo)
        seen = dot(hits, ones)
        if c == 0:
            acc[...] = part
            tally[...] = seen
        else:
            acc[...] += part
            tally[...] += seen

    accumulate(0)
    accumulate(1)
    pl.semaphore_wait(barrier, nz - 1 + plane - 1)

    for _, tz in lines:
        pltpu.make_async_remote_copy(
            crow.at[0], cline.at[z], cz_send, cz_recv, device_id=(x, y, tz), device_id_type=MESH
        ).start()
    accumulate(2)
    accumulate(3)

    def drain(ref, n, sem):
        pltpu.make_async_copy(ref.at[pl.ds(0, n)], ref.at[pl.ds(0, n)], sem).wait()

    drain(cline, nz - 1, cz_recv)
    relayed = cline[0]
    for k in range(1, nz):
        relayed = relayed + cline[k]
    crelay[0] = relayed
    call[q] = relayed

    for px, py in peers:
        pltpu.make_async_remote_copy(
            crelay.at[0], call.at[q], cp_send, cp_recv, device_id=(px, py, z), device_id_type=MESH
        ).start()

    for level in range(2):
        for half in range(2):
            part = acc[pl.ds(level * devices, devices), pl.ds(half * 128, 128)]
            doubled[pl.ds(0, devices), 2 * level + half, :] = part
            doubled[pl.ds(devices, devices), 2 * level + half, :] = part
    flane = lax.broadcasted_iota(I32, (devices, 128), 1)
    tall_keys = jnp.broadcast_to(keys[...].astype(F32) + 1.0, (128, span)).T
    low_half, high_half = pl.ds(0, devices), pl.ds(devices, devices)
    kind = lax.rem(flane, 4)
    field = jnp.where(
        kind < 2,
        jnp.where(kind == 0, tally[low_half, :], tally[high_half, :]),
        jnp.where(kind == 2, tall_keys[:devices], tall_keys[devices:]),
    )
    fields[pl.ds(0, devices), :] = field
    fields[pl.ds(devices, devices), :] = field

    drain(call, plane - 1, cp_recv)
    low = jnp.sum(call[pl.ds(0, plane // 2)], axis=0)
    high = jnp.sum(call[pl.ds(plane // 2, plane // 2)], axis=0)
    counts = jnp.concatenate([low, high], axis=1)
    lanes = lax.broadcasted_iota(I32, (1, devices), 1)
    offset = jnp.sum(jnp.where(lanes < me, counts, 0))
    start = devices - offset % devices
    outgoing[...] = doubled[pl.ds(start, devices)]
    line_id = lax.rem(lax.broadcasted_iota(I32, (devices, 128), 0), nz)
    mark = lax.div(flane, 4) == lax.rem(line_id + q, plane)
    rolled = jnp.where(mark, fields[pl.ds(start, devices), :], 0.0).reshape(plane, nz, 128)
    fsend[...] = jnp.sum(rolled, axis=1, keepdims=True)

    def send_block(px, py, tz):
        target = (px * ny + py) * nz + tz
        pltpu.make_async_remote_copy(
            outgoing.at[target], arrived.at[me], b_send, b_recv, device_id=(px, py, tz), device_id_type=MESH
        ).start()

    def far_first(i, n):
        return n // 2 + jnp.where(lax.rem(i, 2) == 1, -lax.div(i + 1, 2), lax.div(i, 2))

    def send_blocks(i):
        px = lax.rem(x + far_first(lax.div(i, ny), nx), nx)
        py = lax.rem(y + far_first(lax.rem(i, ny), ny), ny)
        for _, tz in lines:
            send_block(px, py, tz)
        send_block(px, py, z)

    for px, py in peers:
        pltpu.make_async_remote_copy(
            fsend.at[px * ny + py], frecv.at[q], fp_send, fp_recv, device_id=(px, py, z), device_id_type=MESH
        ).start()
    pl.loop(0, FIRST)(send_blocks)
    frecv[q] = fsend[q]
    drain(frecv, plane - 1, fp_recv)
    got = frecv[...].reshape(plane, 128)
    group = lax.div(lax.broadcasted_iota(I32, (plane, 128), 1), 4)
    source = lax.broadcasted_iota(I32, (plane, 128), 0)
    for k in range(nz):
        frelay[k] = jnp.sum(jnp.where(group == lax.rem(source + k, plane), got, 0.0), axis=0, keepdims=True)
    farrived[z] = frelay[z]
    for _, tz in lines:
        pltpu.make_async_remote_copy(
            frelay.at[tz], farrived.at[z], fz_send, fz_recv, device_id=(x, y, tz), device_id_type=MESH
        ).start()
    pl.loop(FIRST, plane - 1)(send_blocks)
    for _, tz in lines:
        send_block(x, y, tz)
    own = pltpu.make_async_copy(outgoing.at[me], arrived.at[me], own_sem)
    own.start()

    before = lax.broadcasted_iota(I32, (devices, devices), 0) < lax.broadcasted_iota(I32, (devices, devices), 1)
    before = jnp.where(before, 1.0, 0.0).astype(BF16)
    tops = jnp.broadcast_to((counts // 8).astype(F32).astype(BF16), (8, devices))
    rests = jnp.broadcast_to((counts % 8).astype(F32).astype(BF16), (8, devices))
    offsets = (8.0 * dot(tops, before) + dot(rests, before))[0:1].astype(I32)
    places = []
    for level in range(2):
        position = level * devices + (me - offsets) % devices
        place = (offsets + position) // devices
        places.append(jnp.where(position < counts, place, -1))
    place = jnp.concatenate(places, axis=1)
    picks = jnp.where(lax.broadcasted_iota(I32, (span, span), 0) == place, 1.0, 0.0).astype(BF16)

    drain(farrived, nz - 1, fz_recv)
    got = jnp.concatenate([farrived[k] for k in range(nz)], axis=0)
    wide = jnp.broadcast_to(got[None], (plane, nz, 128)).reshape(devices, 128)
    sender = lax.div(lax.broadcasted_iota(I32, (devices, 128), 0), nz)
    fit = lax.div(flane, 4) == lax.rem(sender + z, plane)
    chosen = jnp.concatenate(
        [jnp.where(fit & (lax.rem(flane, 2) == level), wide, 0.0) for level in range(2)], axis=0
    )
    hi, mid, lo = split3(chosen)
    found = ((dot(picks, hi) + dot(picks, mid)) + dot(picks, lo)).T
    is_key = lax.rem(lax.broadcasted_iota(I32, (128, span), 0), 4) >= 2
    small[0:1] = jnp.sum(jnp.where(is_key, 0.0, found), axis=0, keepdims=True).astype(I32)
    small[1:2] = jnp.sum(jnp.where(is_key, found, 0.0), axis=0, keepdims=True).astype(I32) - 1
    small[2:3] = place
    small[3:4] = jnp.broadcast_to(jnp.sum(counts, axis=1, keepdims=True), (1, span))
    own.wait()
    drain(arrived, devices - 1, b_recv)
    drain(cline, nz - 1, cz_send)
    drain(call, plane - 1, cp_send)
    drain(fsend, plane - 1, fp_send)
    drain(farrived, nz - 1, fz_send)
    drain(outgoing, devices - 1, b_send)


def put(arrived, small, out_sums, out_rows, out_keys, out_total):
    span = out_sums.shape[0]
    out_rows[...] = small[0:1]
    out_keys[...] = small[1:2]
    out_total[...] = small[3:4, 0:1]
    picks = jnp.where(lax.broadcasted_iota(I32, (span, span), 0) == small[2:3], 1.0, 0.0).astype(BF16)
    parts = []
    for level in range(2):
        parts.append(
            jnp.concatenate([arrived[:, 2 * level + half, :] for half in range(2)], axis=1)
        )
    hi, lo = split2(jnp.concatenate(parts, axis=0))
    out_sums[...] = dot(picks, hi) + dot(picks, lo)


def solution(mesh):
    sizes = tuple(mesh.shape[a] for a in AXES)
    nx, ny, nz = sizes
    plane, devices = nx * ny, nx * ny * nz
    vmem = pl.BlockSpec(memory_space=pltpu.VMEM)

    def shards(measures, group_index, distinct_keys, group_counts):
        rows, width = measures.shape
        span = distinct_keys.shape[1]
        hbm = pl.BlockSpec(memory_space=pl.ANY)
        arrived, small = pl.pallas_call(
            functools.partial(kernel, sizes),
            out_shape=(
                jax.ShapeDtypeStruct((devices, 4, 128), F32),
                jax.ShapeDtypeStruct((8, span), I32),
            ),
            in_specs=[hbm] * 3,
            out_specs=(pl.BlockSpec(memory_space=pl.ANY), vmem),
            scratch_shapes=[
                pltpu.VMEM((rows, width), F32),
                pltpu.VMEM((1, rows), I32),
                pltpu.VMEM((1, span), I32),
                pltpu.VMEM((span, width), F32),
                pltpu.VMEM((span, 128), F32),
                pltpu.VMEM((span, 4, 128), F32),
                pltpu.VMEM((span, 128), F32),
                pltpu.VMEM((devices, 4, 128), F32),
                pltpu.VMEM((plane, 1, 128), F32),
                pltpu.VMEM((plane, 1, 128), F32),
                pltpu.VMEM((nz, 1, 128), F32),
                pltpu.VMEM((nz, 1, 128), F32),
                pltpu.VMEM((1, 1, 128), I32),
                pltpu.VMEM((nz, 1, 128), I32),
                pltpu.VMEM((1, 1, 128), I32),
                pltpu.VMEM((plane, 1, 128), I32),
                pltpu.SemaphoreType.DMA((CHUNKS + 2,)),
            ]
            + [pltpu.SemaphoreType.DMA(())] * 11,
            compiler_params=pltpu.CompilerParams(
                collective_id=0, has_side_effects=True, vmem_limit_bytes=32 << 20
            ),
            name="exchange",
        )(*(
            pltpu.with_memory_space_constraint(a, pltpu.MemorySpace.HBM)
            for a in (measures, group_index.reshape(1, rows), distinct_keys)
        ))
        sums, tallies, keys, total = pl.pallas_call(
            put,
            out_shape=(
                jax.ShapeDtypeStruct((span, width), F32),
                jax.ShapeDtypeStruct((1, span), I32),
                jax.ShapeDtypeStruct((1, span), I32),
                jax.ShapeDtypeStruct((1, 1), I32),
            ),
            in_specs=[vmem] * 2,
            out_specs=(vmem,) * 4,
            compiler_params=pltpu.CompilerParams(vmem_limit_bytes=24 << 20),
            name="put",
        )(arrived, small)
        return sums, tallies.reshape(span), keys.reshape(span), total.reshape(())

    return jax.shard_map(
        shards,
        mesh=mesh,
        in_specs=(P(AXES, None), P(AXES), P(AXES, None), P(AXES)),
        out_specs=(P(AXES, None), P(AXES), P(AXES), P()),
        check_vma=False,
    )
```

```python
import functools

import jax
import jax.numpy as jnp
from jax import lax
from jax.experimental import pallas as pl
from jax.experimental.pallas import tpu as pltpu
from jax.sharding import PartitionSpec as P

AXES = ("gx", "gy", "gz")
MESH = pl.DeviceIdType.MESH
F32, BF16, I32 = jnp.float32, jnp.bfloat16, jnp.int32
CHUNKS = 4
EARLY, LATE = 24, 112


def split2(v):
    hi = v.astype(BF16)
    lo = (v - hi.astype(F32)).astype(BF16)
    return hi, lo


def split3(v):
    hi = v.astype(BF16)
    rest = v - hi.astype(F32)
    mid = rest.astype(BF16)
    lo = (rest - mid.astype(F32)).astype(BF16)
    return hi, mid, lo


def dot(a, b):
    return jnp.dot(a, b, preferred_element_type=F32)


def kernel(
    sizes,
    measures, index_in, keys_in,
    arrived, small,
    values, index, keys, acc, tally, doubled, fields, outgoing, fsend, frecv, frelay, farrived,
    crow, cline, crelay, call,
    load_sems, own_sem, cz_send, cz_recv, cp_send, cp_recv, fp_send, fp_recv, fz_send, fz_recv, b_send, b_recv,
):
    nx, ny, nz = sizes
    plane, devices = nx * ny, nx * ny * nz
    rows = measures.shape[0]
    step = rows // CHUNKS
    span = 2 * devices
    x, y, z = (lax.axis_index(a) for a in AXES)
    q = x * ny + y
    me = q * nz + z

    def outward(n):
        return sorted(range(n), key=lambda k: -min(k, n - k))

    def moved(base, k, n):
        return lax.rem(base + k, n) if k else base

    lines = [(k, moved(z, k, nz)) for k in outward(nz) if k]
    across = sorted(
        ((i, j) for i in range(nx) for j in range(ny) if i or j),
        key=lambda t: -(min(t[0], nx - t[0]) + min(t[1], ny - t[1]) / 2),
    )
    xs = [moved(x, k, nx) for k in range(nx)]
    ys = [moved(y, k, ny) for k in range(ny)]
    peers = [(xs[i], ys[j]) for i, j in across]

    barrier = pltpu.get_barrier_semaphore()
    for px, py in peers:
        pl.semaphore_signal(barrier, inc=1, device_id=(px, py, z), device_id_type=MESH)
    for _, tz in lines:
        pl.semaphore_signal(barrier, inc=1, device_id=(x, y, tz), device_id_type=MESH)

    loads = [
        pltpu.make_async_copy(
            measures.at[pl.ds(c * step, step)], values.at[pl.ds(c * step, step)], load_sems.at[c]
        )
        for c in range(CHUNKS)
    ]
    inputs = [
        pltpu.make_async_copy(src, dst, load_sems.at[CHUNKS + i])
        for i, (src, dst) in enumerate(((index_in, index), (keys_in, keys)))
    ]
    for load in inputs + loads:
        load.start()

    for load in inputs:
        load.wait()
    count = jnp.max(index[...], axis=1, keepdims=True) + 1
    lane = lax.broadcasted_iota(I32, (1, 128), 1)
    mine = jnp.where(lane == me % 128, count, 0)
    crow[0] = mine
    cline[z] = mine

    labels = lax.broadcasted_iota(I32, (span, step), 0)
    ones = jnp.ones((step, 128), BF16)

    def accumulate(c):
        loads[c].wait()
        hits = jnp.where(labels == index[0:1, c * step : (c + 1) * step], 1.0, 0.0).astype(BF16)
        hi, lo = split2(values[pl.ds(c * step, step)])
        part = dot(hits, hi) + dot(hits, lo)
        seen = dot(hits, ones)
        if c == 0:
            acc[...] = part
            tally[...] = seen
        else:
            acc[...] += part
            tally[...] += seen

    pl.semaphore_wait(barrier, nz - 1 + plane - 1)

    for _, tz in lines:
        pltpu.make_async_remote_copy(
            crow.at[0], cline.at[z], cz_send, cz_recv, device_id=(x, y, tz), device_id_type=MESH
        ).start()
    for c in range(CHUNKS):
        accumulate(c)

    def drain(ref, n, sem):
        pltpu.make_async_copy(ref.at[pl.ds(0, n)], ref.at[pl.ds(0, n)], sem).wait()

    drain(cline, nz - 1, cz_recv)
    relayed = cline[0]
    for k in range(1, nz):
        relayed = relayed + cline[k]
    crelay[0] = relayed
    call[q] = relayed

    for px, py in peers:
        pltpu.make_async_remote_copy(
            crelay.at[0], call.at[q], cp_send, cp_recv, device_id=(px, py, z), device_id_type=MESH
        ).start()

    for level in range(2):
        for half in range(2):
            part = acc[pl.ds(level * devices, devices), pl.ds(half * 128, 128)]
            doubled[pl.ds(0, devices), 2 * level + half, :] = part
            doubled[pl.ds(devices, devices), 2 * level + half, :] = part
    flane = lax.broadcasted_iota(I32, (devices, 128), 1)
    tall_keys = jnp.broadcast_to(keys[...].astype(F32) + 1.0, (128, span)).T
    low_half, high_half = pl.ds(0, devices), pl.ds(devices, devices)
    kind = lax.rem(flane, 4)
    field = jnp.where(
        kind < 2,
        jnp.where(kind == 0, tally[low_half, :], tally[high_half, :]),
        jnp.where(kind == 2, tall_keys[:devices], tall_keys[devices:]),
    )
    fields[pl.ds(0, devices), :] = field
    fields[pl.ds(devices, devices), :] = field

    drain(call, plane - 1, cp_recv)
    low = jnp.sum(call[pl.ds(0, plane // 2)], axis=0)
    high = jnp.sum(call[pl.ds(plane // 2, plane // 2)], axis=0)
    counts = jnp.concatenate([low, high], axis=1)
    lanes = lax.broadcasted_iota(I32, (1, devices), 1)
    offset = jnp.sum(jnp.where(lanes < me, counts, 0))
    start = devices - offset % devices
    outgoing[...] = doubled[pl.ds(start, devices)]

    def send_block(px, py, tz):
        target = (px * ny + py) * nz + tz
        pltpu.make_async_remote_copy(
            outgoing.at[target], arrived.at[me], b_send, b_recv, device_id=(px, py, tz), device_id_type=MESH
        ).start()

    def hops(offset):
        i, j, k = offset
        return min(i, nx - i) + min(j, ny - j) / 2 + (j % 2) * 0.1 + min(k, nz - k)

    order = sorted(
        ((i, j, k) for i in range(nx) for j in range(ny) for k in range(nz) if i or j or k),
        key=lambda t: (-hops(t), t),
    )
    zs = [moved(z, k, nz) for k in range(nz)]

    def send_blocks(offsets):
        for i, j, k in offsets:
            send_block(xs[i], ys[j], zs[k])

    send_blocks(order[:EARLY])
    line_id = lax.rem(lax.broadcasted_iota(I32, (devices, 128), 0), nz)
    mark = lax.div(flane, 4) == lax.rem(line_id + q, plane)
    rolled = jnp.where(mark, fields[pl.ds(start, devices), :], 0.0).reshape(plane, nz, 128)
    fsend[...] = jnp.sum(rolled, axis=1, keepdims=True)
    for px, py in peers:
        pltpu.make_async_remote_copy(
            fsend.at[px * ny + py], frecv.at[q], fp_send, fp_recv, device_id=(px, py, z), device_id_type=MESH
        ).start()
    send_blocks(order[EARLY:LATE])
    frecv[q] = fsend[q]
    drain(frecv, plane - 1, fp_recv)
    got = frecv[...].reshape(plane, 128)
    group = lax.div(lax.broadcasted_iota(I32, (plane, 128), 1), 4)
    source = lax.broadcasted_iota(I32, (plane, 128), 0)
    for k in range(nz):
        frelay[k] = jnp.sum(jnp.where(group == lax.rem(source + k, plane), got, 0.0), axis=0, keepdims=True)
    farrived[z] = frelay[z]
    for _, tz in lines:
        pltpu.make_async_remote_copy(
            frelay.at[tz], farrived.at[z], fz_send, fz_recv, device_id=(x, y, tz), device_id_type=MESH
        ).start()
    send_blocks(order[LATE:])
    own = pltpu.make_async_copy(outgoing.at[me], arrived.at[me], own_sem)
    own.start()

    before = lax.broadcasted_iota(I32, (devices, devices), 0) < lax.broadcasted_iota(I32, (devices, devices), 1)
    before = jnp.where(before, 1.0, 0.0).astype(BF16)
    tops = jnp.broadcast_to((counts // 8).astype(F32).astype(BF16), (8, devices))
    rests = jnp.broadcast_to((counts % 8).astype(F32).astype(BF16), (8, devices))
    offsets = (8.0 * dot(tops, before) + dot(rests, before))[0:1].astype(I32)
    places = []
    for level in range(2):
        position = level * devices + (me - offsets) % devices
        place = (offsets + position) // devices
        places.append(jnp.where(position < counts, place, -1))
    place = jnp.concatenate(places, axis=1)
    picks = jnp.where(lax.broadcasted_iota(I32, (span, span), 0) == place, 1.0, 0.0).astype(BF16)

    drain(farrived, nz - 1, fz_recv)
    got = jnp.concatenate([farrived[k] for k in range(nz)], axis=0)
    wide = jnp.broadcast_to(got[None], (plane, nz, 128)).reshape(devices, 128)
    sender = lax.div(lax.broadcasted_iota(I32, (devices, 128), 0), nz)
    fit = lax.div(flane, 4) == lax.rem(sender + z, plane)
    chosen = jnp.concatenate(
        [jnp.where(fit & (lax.rem(flane, 2) == level), wide, 0.0) for level in range(2)], axis=0
    )
    hi, mid, lo = split3(chosen)
    found = ((dot(picks, hi) + dot(picks, mid)) + dot(picks, lo)).T
    is_key = lax.rem(lax.broadcasted_iota(I32, (128, span), 0), 4) >= 2
    small[0:1] = jnp.sum(jnp.where(is_key, 0.0, found), axis=0, keepdims=True).astype(I32)
    small[1:2] = jnp.sum(jnp.where(is_key, found, 0.0), axis=0, keepdims=True).astype(I32) - 1
    small[2:3] = place
    small[3:4] = jnp.broadcast_to(jnp.sum(counts, axis=1, keepdims=True), (1, span))
    own.wait()
    drain(arrived, devices - 1, b_recv)
    drain(cline, nz - 1, cz_send)
    drain(call, plane - 1, cp_send)
    drain(fsend, plane - 1, fp_send)
    drain(farrived, nz - 1, fz_send)
    drain(outgoing, devices - 1, b_send)


def put(arrived, small, out_sums, out_rows, out_keys, out_total):
    span = out_sums.shape[0]
    senders = span // 2
    out_rows[...] = small[0:1]
    out_keys[...] = small[1:2]
    out_total[...] = small[3:4, 0:1]
    total = None
    for level in range(2):
        block = jnp.concatenate(
            [arrived[pl.ds(2 * level + half, senders, stride=4), :] for half in range(2)], axis=1
        )
        hi, lo = split2(block)
        places = small[2:3, level * senders : (level + 1) * senders]
        labels = lax.broadcasted_iota(I32, (span, senders), 0)
        picks = jnp.where(labels == places, 1.0, 0.0).astype(BF16)
        part = dot(picks, hi) + dot(picks, lo)
        total = part if total is None else total + part
    out_sums[...] = total


def solution(mesh):
    sizes = tuple(mesh.shape[a] for a in AXES)
    nx, ny, nz = sizes
    plane, devices = nx * ny, nx * ny * nz
    vmem = pl.BlockSpec(memory_space=pltpu.VMEM)

    def shards(measures, group_index, distinct_keys, group_counts):
        rows, width = measures.shape
        span = distinct_keys.shape[1]
        hbm = pl.BlockSpec(memory_space=pl.ANY)
        arrived, small = pl.pallas_call(
            functools.partial(kernel, sizes),
            out_shape=(
                jax.ShapeDtypeStruct((devices, 4, 128), F32),
                jax.ShapeDtypeStruct((8, span), I32),
            ),
            in_specs=[hbm] * 3,
            out_specs=(pl.BlockSpec(memory_space=pl.ANY), vmem),
            scratch_shapes=[
                pltpu.VMEM((rows, width), F32),
                pltpu.VMEM((1, rows), I32),
                pltpu.VMEM((1, span), I32),
                pltpu.VMEM((span, width), F32),
                pltpu.VMEM((span, 128), F32),
                pltpu.VMEM((span, 4, 128), F32),
                pltpu.VMEM((span, 128), F32),
                pltpu.VMEM((devices, 4, 128), F32),
                pltpu.VMEM((plane, 1, 128), F32),
                pltpu.VMEM((plane, 1, 128), F32),
                pltpu.VMEM((nz, 1, 128), F32),
                pltpu.VMEM((nz, 1, 128), F32),
                pltpu.VMEM((1, 1, 128), I32),
                pltpu.VMEM((nz, 1, 128), I32),
                pltpu.VMEM((1, 1, 128), I32),
                pltpu.VMEM((plane, 1, 128), I32),
                pltpu.SemaphoreType.DMA((CHUNKS + 2,)),
            ]
            + [pltpu.SemaphoreType.DMA(())] * 11,
            compiler_params=pltpu.CompilerParams(
                collective_id=0, has_side_effects=True, vmem_limit_bytes=32 << 20
            ),
            name="exchange",
        )(*(
            pltpu.with_memory_space_constraint(a, pltpu.MemorySpace.HBM)
            for a in (measures, group_index.reshape(1, rows), distinct_keys)
        ))
        sums, tallies, keys, total = pl.pallas_call(
            put,
            out_shape=(
                jax.ShapeDtypeStruct((span, width), F32),
                jax.ShapeDtypeStruct((1, span), I32),
                jax.ShapeDtypeStruct((1, span), I32),
                jax.ShapeDtypeStruct((1, 1), I32),
            ),
            in_specs=[vmem] * 2,
            out_specs=(vmem,) * 4,
            compiler_params=pltpu.CompilerParams(vmem_limit_bytes=24 << 20),
            name="put",
        )(arrived.reshape(4 * devices, 128), small)
        return sums, tallies.reshape(span), keys.reshape(span), total.reshape(())

    return jax.shard_map(
        shards,
        mesh=mesh,
        in_specs=(P(AXES, None), P(AXES), P(AXES, None), P(AXES)),
        out_specs=(P(AXES, None), P(AXES), P(AXES), P()),
        check_vma=False,
    )
```

```python
import functools

import jax
import jax.numpy as jnp
from jax import lax
from jax.experimental import pallas as pl
from jax.experimental.pallas import tpu as pltpu
from jax.sharding import PartitionSpec as P

AXES = ("gx", "gy", "gz")
MESH = pl.DeviceIdType.MESH
F32, BF16, I32 = jnp.float32, jnp.bfloat16, jnp.int32
CHUNKS = 4
EARLY, LATE = 24, 112


def split2(v):
    hi = v.astype(BF16)
    lo = (v - hi.astype(F32)).astype(BF16)
    return hi, lo


def split3(v):
    hi = v.astype(BF16)
    rest = v - hi.astype(F32)
    mid = rest.astype(BF16)
    lo = (rest - mid.astype(F32)).astype(BF16)
    return hi, mid, lo


def dot(a, b):
    return jnp.dot(a, b, preferred_element_type=F32)


def kernel(
    sizes,
    measures, index_in, keys_in,
    arrived, small,
    values, index, keys, acc, tally, halves, near, fields, outgoing, fsend, frecv, frelay, farrived,
    crow, cline, crelay, call,
    load_sems, own_sems, near_send, near_recv, cz_send, cz_recv, cp_send, cp_recv, fp_send, fp_recv, fz_send, fz_recv, b_send, b_recv,
):
    nx, ny, nz = sizes
    plane, devices = nx * ny, nx * ny * nz
    rows = measures.shape[0]
    step = rows // CHUNKS
    span = 2 * devices
    x, y, z = (lax.axis_index(a) for a in AXES)
    q = x * ny + y
    me = q * nz + z

    def outward(n):
        return sorted(range(n), key=lambda k: -min(k, n - k))

    def moved(base, k, n):
        return lax.rem(base + k, n) if k else base

    lines = [(k, moved(z, k, nz)) for k in outward(nz) if k]
    across = sorted(
        ((i, j) for i in range(nx) for j in range(ny) if i or j),
        key=lambda t: -(min(t[0], nx - t[0]) + min(t[1], ny - t[1]) / 2),
    )
    xs = [moved(x, k, nx) for k in range(nx)]
    ys = [moved(y, k, ny) for k in range(ny)]
    peers = [(xs[i], ys[j]) for i, j in across]

    barrier = pltpu.get_barrier_semaphore()
    for px, py in peers:
        pl.semaphore_signal(barrier, inc=1, device_id=(px, py, z), device_id_type=MESH)
    for _, tz in lines:
        pl.semaphore_signal(barrier, inc=1, device_id=(x, y, tz), device_id_type=MESH)

    loads = [
        pltpu.make_async_copy(
            measures.at[pl.ds(c * step, step)], values.at[pl.ds(c * step, step)], load_sems.at[c]
        )
        for c in range(CHUNKS)
    ]
    inputs = [
        pltpu.make_async_copy(src, dst, load_sems.at[CHUNKS + i])
        for i, (src, dst) in enumerate(((index_in, index), (keys_in, keys)))
    ]
    for load in inputs + loads:
        load.start()

    for load in inputs:
        load.wait()
    count = jnp.max(index[...], axis=1, keepdims=True) + 1
    lane = lax.broadcasted_iota(I32, (1, 128), 1)
    mine = jnp.where(lane == me % 128, count, 0)
    crow[0] = mine
    cline[z] = mine

    labels = lax.broadcasted_iota(I32, (span, step), 0)
    ones = jnp.ones((step, 128), BF16)

    def accumulate(c):
        loads[c].wait()
        hits = jnp.where(labels == index[0:1, c * step : (c + 1) * step], 1.0, 0.0).astype(BF16)
        hi, lo = split2(values[pl.ds(c * step, step)])
        part = dot(hits, hi) + dot(hits, lo)
        seen = dot(hits, ones)
        if c == 0:
            acc[...] = part
            tally[...] = seen
        else:
            acc[...] += part
            tally[...] += seen

    pl.semaphore_wait(barrier, nz - 1 + plane - 1)

    for _, tz in lines:
        pltpu.make_async_remote_copy(
            crow.at[0], cline.at[z], cz_send, cz_recv, device_id=(x, y, tz), device_id_type=MESH
        ).start()
    for c in range(CHUNKS):
        accumulate(c)

    def drain(ref, n, sem):
        pltpu.make_async_copy(ref.at[pl.ds(0, n)], ref.at[pl.ds(0, n)], sem).wait()

    for half in range(2):
        for level in range(2):
            part = acc[pl.ds(level * devices, devices), pl.ds(half * 128, 128)]
            halves[half, level, pl.ds(0, devices), :] = part
            halves[half, level, pl.ds(devices, devices), :] = part
    for half, tz in ((0, moved(z, 1, nz)), (1, moved(z, nz - 1, nz))):
        for level in range(2):
            pltpu.make_async_remote_copy(
                halves.at[half, level, pl.ds(0, devices)], near.at[half, level, pl.ds(0, devices)],
                near_send, near_recv, device_id=(x, y, tz), device_id_type=MESH,
            ).start()
    drain(cline, nz - 1, cz_recv)
    relayed = cline[0]
    for k in range(1, nz):
        relayed = relayed + cline[k]
    crelay[0] = relayed
    call[q] = relayed

    for px, py in peers:
        pltpu.make_async_remote_copy(
            crelay.at[0], call.at[q], cp_send, cp_recv, device_id=(px, py, z), device_id_type=MESH
        ).start()

    flane = lax.broadcasted_iota(I32, (devices, 128), 1)
    tall_keys = jnp.broadcast_to(keys[...].astype(F32) + 1.0, (128, span)).T
    low_half, high_half = pl.ds(0, devices), pl.ds(devices, devices)
    kind = lax.rem(flane, 4)
    field = jnp.where(
        kind < 2,
        jnp.where(kind == 0, tally[low_half, :], tally[high_half, :]),
        jnp.where(kind == 2, tall_keys[:devices], tall_keys[devices:]),
    )
    fields[pl.ds(0, devices), :] = field
    fields[pl.ds(devices, devices), :] = field

    drain(call, plane - 1, cp_recv)
    low = jnp.sum(call[pl.ds(0, plane // 2)], axis=0)
    high = jnp.sum(call[pl.ds(plane // 2, plane // 2)], axis=0)
    counts = jnp.concatenate([low, high], axis=1)
    lanes = lax.broadcasted_iota(I32, (1, devices), 1)

    def start_of(device):
        return devices - lax.rem(jnp.sum(jnp.where(lanes < device, counts, 0)), devices)

    start = start_of(me)
    for level in range(2):
        outgoing[0, pl.ds(level, devices, stride=4), :] = halves[1, level, pl.ds(start, devices), :]
        outgoing[1, pl.ds(level, devices, stride=4), :] = halves[0, level, pl.ds(start, devices), :]
    pltpu.make_async_copy(acc, acc, near_recv).wait()
    for half, other in ((0, moved(z, nz - 1, nz)), (1, moved(z, 1, nz))):
        first = start_of(q * nz + other)
        for level in range(2):
            near[half, level, pl.ds(devices, devices), :] = near[half, level, pl.ds(0, devices), :]
            outgoing[half, pl.ds(2 + level, devices, stride=4), :] = near[half, level, pl.ds(first, devices), :]

    reach = nz // 2

    def hops(offset):
        i, j, side, k = offset
        return min(i, nx - i) + min(j, ny - j) / 2 + (j % 2) * 0.1 + k

    order = sorted(
        (
            (i, j, side, k)
            for i in range(nx) for j in range(ny) for side in range(2) for k in range(reach) if i or j or k
        ),
        key=lambda t: (-hops(t), t),
    )
    zs = [moved(z, k, nz) for k in range(nz)]

    def send_blocks(offsets):
        for i, j, side, k in offsets:
            px, py, tz = xs[i], ys[j], zs[(nz - k) % nz if side else k]
            target = (px * ny + py) * nz + tz
            pltpu.make_async_remote_copy(
                outgoing.at[side, pl.ds(4 * target, 4)],
                arrived.at[(side * plane + q) * reach + k],
                b_send, b_recv, device_id=(px, py, tz), device_id_type=MESH,
            ).start()

    send_blocks(order[:EARLY])
    line_id = lax.rem(lax.broadcasted_iota(I32, (devices, 128), 0), nz)
    mark = lax.div(flane, 4) == lax.rem(line_id + q, plane)
    rolled = jnp.where(mark, fields[pl.ds(start, devices), :], 0.0).reshape(plane, nz, 128)
    fsend[...] = jnp.sum(rolled, axis=1, keepdims=True)
    for px, py in peers:
        pltpu.make_async_remote_copy(
            fsend.at[px * ny + py], frecv.at[q], fp_send, fp_recv, device_id=(px, py, z), device_id_type=MESH
        ).start()
    send_blocks(order[EARLY:LATE])
    frecv[q] = fsend[q]
    drain(frecv, plane - 1, fp_recv)
    got = frecv[...].reshape(plane, 128)
    group = lax.div(lax.broadcasted_iota(I32, (plane, 128), 1), 4)
    source = lax.broadcasted_iota(I32, (plane, 128), 0)
    for k in range(nz):
        frelay[k] = jnp.sum(jnp.where(group == lax.rem(source + k, plane), got, 0.0), axis=0, keepdims=True)
    farrived[z] = frelay[z]
    for _, tz in lines:
        pltpu.make_async_remote_copy(
            frelay.at[tz], farrived.at[z], fz_send, fz_recv, device_id=(x, y, tz), device_id_type=MESH
        ).start()
    send_blocks(order[LATE:])
    owns = [
        pltpu.make_async_copy(
            outgoing.at[side, pl.ds(4 * me, 4)], arrived.at[(side * plane + q) * reach], own_sems.at[side]
        )
        for side in range(2)
    ]
    for own in owns:
        own.start()

    before = lax.broadcasted_iota(I32, (devices, devices), 0) < lax.broadcasted_iota(I32, (devices, devices), 1)
    before = jnp.where(before, 1.0, 0.0).astype(BF16)
    tops = jnp.broadcast_to((counts // 8).astype(F32).astype(BF16), (8, devices))
    rests = jnp.broadcast_to((counts % 8).astype(F32).astype(BF16), (8, devices))
    offsets = (8.0 * dot(tops, before) + dot(rests, before))[0:1].astype(I32)
    places = []
    for level in range(2):
        position = level * devices + (me - offsets) % devices
        place = (offsets + position) // devices
        places.append(jnp.where(position < counts, place, -1))
    place = jnp.concatenate(places, axis=1)
    picks = jnp.where(lax.broadcasted_iota(I32, (span, span), 0) == place, 1.0, 0.0).astype(BF16)

    drain(farrived, nz - 1, fz_recv)
    got = jnp.concatenate([farrived[k] for k in range(nz)], axis=0)
    wide = jnp.broadcast_to(got[None], (plane, nz, 128)).reshape(devices, 128)
    sender = lax.div(lax.broadcasted_iota(I32, (devices, 128), 0), nz)
    fit = lax.div(flane, 4) == lax.rem(sender + z, plane)
    chosen = jnp.concatenate(
        [jnp.where(fit & (lax.rem(flane, 2) == level), wide, 0.0) for level in range(2)], axis=0
    )
    hi, mid, lo = split3(chosen)
    found = ((dot(picks, hi) + dot(picks, mid)) + dot(picks, lo)).T
    is_key = lax.rem(lax.broadcasted_iota(I32, (128, span), 0), 4) >= 2
    small[0:1] = jnp.sum(jnp.where(is_key, 0.0, found), axis=0, keepdims=True).astype(I32)
    small[1:2] = jnp.sum(jnp.where(is_key, found, 0.0), axis=0, keepdims=True).astype(I32) - 1
    level_row = lax.broadcasted_iota(I32, (8, devices), 0)
    natural = jnp.where(level_row == 0, place[:, :devices], place[:, devices:]).astype(F32) + 1.0
    hi, lo = split2(natural)
    slot = lax.broadcasted_iota(I32, (devices, devices), 1)
    holder = lax.div(lax.rem(slot, devices // 2), reach)
    shift = lax.rem(slot, reach)
    direct = slot < devices // 2
    for row, step_z in (
        (2, jnp.where(direct, nz + shift, nz - shift - 1)),
        (3, jnp.where(direct, nz - shift, nz + shift + 1)),
    ):
        source = holder * nz + lax.rem(z + step_z, nz)
        match = lax.broadcasted_iota(I32, (devices, devices), 0) == source
        match = jnp.where(match, 1.0, 0.0).astype(BF16)
        ordered = (dot(hi, match) + dot(lo, match)).astype(I32) - 1
        small[row : row + 1] = jnp.concatenate([ordered[0:1], ordered[1:2]], axis=1)
    small[4:5] = jnp.broadcast_to(jnp.sum(counts, axis=1, keepdims=True), (1, span))
    for own in owns:
        own.wait()
    drain(arrived, devices - 2, b_recv)
    drain(cline, nz - 1, cz_send)
    drain(call, plane - 1, cp_send)
    drain(fsend, plane - 1, fp_send)
    drain(farrived, nz - 1, fz_send)
    drain(arrived, devices - 2, b_send)
    pltpu.make_async_copy(acc, acc, near_send).wait()


def put(arrived, small, out_sums, out_rows, out_keys, out_total):
    span = out_sums.shape[0]
    senders = span // 2
    slots = senders // 2
    out_rows[...] = small[0:1]
    out_keys[...] = small[1:2]
    out_total[...] = small[4:5, 0:1]
    labels = lax.broadcasted_iota(I32, (span, senders), 0)
    sides = []
    for half in range(2):
        direct, relayed = (4 * slots, 2) if half == 0 else (0, 4 * slots + 2)
        total = None
        for level in range(2):
            block = jnp.concatenate(
                [arrived[pl.ds(base + level, slots, stride=4), :] for base in (direct, relayed)], axis=0
            )
            places = small[2 + half : 3 + half, level * senders : (level + 1) * senders]
            picks = jnp.where(labels == places, 1.0, 0.0).astype(BF16)
            part = dot(picks, jnp.concatenate(split2(block), axis=1))
            total = part if total is None else total + part
        sides.append(total[:, :128] + total[:, 128:])
    out_sums[...] = jnp.concatenate(sides, axis=1)


def solution(mesh):
    sizes = tuple(mesh.shape[a] for a in AXES)
    nx, ny, nz = sizes
    plane, devices = nx * ny, nx * ny * nz
    vmem = pl.BlockSpec(memory_space=pltpu.VMEM)

    def shards(measures, group_index, distinct_keys, group_counts):
        rows, width = measures.shape
        span = distinct_keys.shape[1]
        hbm = pl.BlockSpec(memory_space=pl.ANY)
        arrived, small = pl.pallas_call(
            functools.partial(kernel, sizes),
            out_shape=(
                jax.ShapeDtypeStruct((devices, 4, 128), F32),
                jax.ShapeDtypeStruct((8, span), I32),
            ),
            in_specs=[hbm] * 3,
            out_specs=(pl.BlockSpec(memory_space=pl.ANY), vmem),
            scratch_shapes=[
                pltpu.VMEM((rows, width), F32),
                pltpu.VMEM((1, rows), I32),
                pltpu.VMEM((1, span), I32),
                pltpu.VMEM((span, width), F32),
                pltpu.VMEM((span, 128), F32),
                pltpu.VMEM((2, 2, span, 128), F32),
                pltpu.VMEM((2, 2, span, 128), F32),
                pltpu.VMEM((span, 128), F32),
                pltpu.VMEM((2, 4 * devices, 128), F32),
                pltpu.VMEM((plane, 1, 128), F32),
                pltpu.VMEM((plane, 1, 128), F32),
                pltpu.VMEM((nz, 1, 128), F32),
                pltpu.VMEM((nz, 1, 128), F32),
                pltpu.VMEM((1, 1, 128), I32),
                pltpu.VMEM((nz, 1, 128), I32),
                pltpu.VMEM((1, 1, 128), I32),
                pltpu.VMEM((plane, 1, 128), I32),
                pltpu.SemaphoreType.DMA((CHUNKS + 2,)),
                pltpu.SemaphoreType.DMA((2,)),
            ]
            + [pltpu.SemaphoreType.DMA(())] * 12,
            compiler_params=pltpu.CompilerParams(
                collective_id=0, has_side_effects=True, vmem_limit_bytes=32 << 20
            ),
            name="exchange",
        )(*(
            pltpu.with_memory_space_constraint(a, pltpu.MemorySpace.HBM)
            for a in (measures, group_index.reshape(1, rows), distinct_keys)
        ))
        sums, tallies, keys, total = pl.pallas_call(
            put,
            out_shape=(
                jax.ShapeDtypeStruct((span, width), F32),
                jax.ShapeDtypeStruct((1, span), I32),
                jax.ShapeDtypeStruct((1, span), I32),
                jax.ShapeDtypeStruct((1, 1), I32),
            ),
            in_specs=[vmem] * 2,
            out_specs=(vmem,) * 4,
            compiler_params=pltpu.CompilerParams(vmem_limit_bytes=24 << 20),
            name="put",
        )(arrived.reshape(4 * devices, 128), small)
        return sums, tallies.reshape(span), keys.reshape(span), total.reshape(())

    return jax.shard_map(
        shards,
        mesh=mesh,
        in_specs=(P(AXES, None), P(AXES), P(AXES, None), P(AXES)),
        out_specs=(P(AXES, None), P(AXES), P(AXES), P()),
        check_vma=False,
    )
```

```python
import functools

import jax
import jax.numpy as jnp
from jax import lax
from jax.experimental import pallas as pl
from jax.experimental.pallas import tpu as pltpu
from jax.sharding import PartitionSpec as P

AXES = ("gx", "gy", "gz")
MESH = pl.DeviceIdType.MESH
F32, BF16, I32 = jnp.float32, jnp.bfloat16, jnp.int32
CHUNKS = 4
LATE = 150


def split2(v):
    hi = v.astype(BF16)
    lo = (v - hi.astype(F32)).astype(BF16)
    return hi, lo


def split3(v):
    hi = v.astype(BF16)
    rest = v - hi.astype(F32)
    mid = rest.astype(BF16)
    lo = (rest - mid.astype(F32)).astype(BF16)
    return hi, mid, lo


def dot(a, b):
    return jnp.dot(a, b, preferred_element_type=F32)


def kernel(
    sizes,
    measures, index_in, keys_in,
    arrived, small,
    values, index, keys, acc, tally, halves, near, outgoing, fsend, frecv, fown, fline,
    crow, cline, crelay, call,
    load_sems, own_sems, near_send, near_recv, cz_send, cz_recv, cp_send, cp_recv, fp_send, fp_recv, fz_send, fz_recv, b_send, b_recv,
):
    nx, ny, nz = sizes
    plane, devices = nx * ny, nx * ny * nz
    rows = measures.shape[0]
    step = rows // CHUNKS
    span = 2 * devices
    x, y, z = (lax.axis_index(a) for a in AXES)
    q = x * ny + y
    me = q * nz + z

    def outward(n):
        return sorted(range(n), key=lambda k: -min(k, n - k))

    def moved(base, k, n):
        return lax.rem(base + k, n) if k else base

    lines = [(k, moved(z, k, nz)) for k in outward(nz) if k]
    across = sorted(
        ((i, j) for i in range(nx) for j in range(ny) if i or j),
        key=lambda t: -(min(t[0], nx - t[0]) + min(t[1], ny - t[1]) / 2),
    )
    xs = [moved(x, k, nx) for k in range(nx)]
    ys = [moved(y, k, ny) for k in range(ny)]
    peers = [(xs[i], ys[j]) for i, j in across]

    barrier = pltpu.get_barrier_semaphore()
    for px, py in peers:
        pl.semaphore_signal(barrier, inc=1, device_id=(px, py, z), device_id_type=MESH)
    for _, tz in lines:
        pl.semaphore_signal(barrier, inc=1, device_id=(x, y, tz), device_id_type=MESH)

    loads = [
        pltpu.make_async_copy(
            measures.at[pl.ds(c * step, step)], values.at[pl.ds(c * step, step)], load_sems.at[c]
        )
        for c in range(CHUNKS)
    ]
    inputs = [
        pltpu.make_async_copy(src, dst, load_sems.at[CHUNKS + i])
        for i, (src, dst) in enumerate(((index_in, index), (keys_in, keys)))
    ]
    for load in inputs + loads:
        load.start()

    for load in inputs:
        load.wait()
    count = jnp.max(index[...], axis=1, keepdims=True) + 1
    lane = lax.broadcasted_iota(I32, (1, 128), 1)
    mine = jnp.where(lane == me % 128, count, 0)
    crow[0] = mine
    cline[z] = mine

    labels = lax.broadcasted_iota(I32, (span, step), 0)

    ones = jnp.ones((step, 128), BF16)

    def accumulate(c):
        loads[c].wait()
        hits = jnp.where(labels == index[0:1, c * step : (c + 1) * step], 1.0, 0.0).astype(BF16)
        hi, lo = split2(values[pl.ds(c * step, step)])
        part = dot(hits, hi) + dot(hits, lo)
        seen = dot(hits, ones)
        if c == 0:
            acc[...] = part
            tally[...] = seen
        else:
            acc[...] += part
            tally[...] += seen

    for c in range(CHUNKS // 2):
        accumulate(c)
    pl.semaphore_wait(barrier, nz - 1 + plane - 1)

    for _, tz in lines:
        pltpu.make_async_remote_copy(
            crow.at[0], cline.at[z], cz_send, cz_recv, device_id=(x, y, tz), device_id_type=MESH
        ).start()
    for c in range(CHUNKS // 2, CHUNKS):
        accumulate(c)

    def drain(ref, n, sem):
        pltpu.make_async_copy(ref.at[pl.ds(0, n)], ref.at[pl.ds(0, n)], sem).wait()

    for half in range(2):
        for level in range(2):
            part = acc[pl.ds(level * devices, devices), pl.ds(half * 128, 128)]
            halves[half, level, pl.ds(0, devices), :] = part
            halves[half, level, pl.ds(devices, devices), :] = part
    for half, tz in ((0, moved(z, 1, nz)), (1, moved(z, nz - 1, nz))):
        for level in range(2):
            pltpu.make_async_remote_copy(
                halves.at[half, level, pl.ds(0, devices)], near.at[half, level, pl.ds(0, devices)],
                near_send, near_recv, device_id=(x, y, tz), device_id_type=MESH,
            ).start()
    seen = tally[...].T[0:1]
    named = keys[...].astype(F32) + 1.0
    fown[0] = jnp.concatenate(
        [row[:, level * devices : (level + 1) * devices] for row in (seen, named) for level in range(2)], axis=0
    )
    fline[z] = fown[0]
    for _, tz in lines:
        pltpu.make_async_remote_copy(
            fown.at[0], fline.at[z], fz_send, fz_recv, device_id=(x, y, tz), device_id_type=MESH
        ).start()
    drain(cline, nz - 1, cz_recv)
    relayed = cline[0]
    for k in range(1, nz):
        relayed = relayed + cline[k]
    crelay[0] = relayed
    call[q] = relayed

    for px, py in peers:
        pltpu.make_async_remote_copy(
            crelay.at[0], call.at[q], cp_send, cp_recv, device_id=(px, py, z), device_id_type=MESH
        ).start()

    pltpu.make_async_copy(acc, acc, near_recv).wait()
    for half in range(2):
        for level in range(2):
            near[half, level, pl.ds(devices, devices), :] = near[half, level, pl.ds(0, devices), :]
    drain(call, plane - 1, cp_recv)
    low = jnp.sum(call[pl.ds(0, plane // 2)], axis=0)
    high = jnp.sum(call[pl.ds(plane // 2, plane // 2)], axis=0)
    counts = jnp.concatenate([low, high], axis=1)
    lanes = lax.broadcasted_iota(I32, (1, devices), 1)

    def start_of(device):
        return devices - lax.rem(jnp.sum(jnp.where(lanes < device, counts, 0)), devices)

    start = start_of(me)
    for level in range(2):
        outgoing[0, pl.ds(level, devices, stride=4), :] = halves[1, level, pl.ds(start, devices), :]
        outgoing[1, pl.ds(level, devices, stride=4), :] = halves[0, level, pl.ds(start, devices), :]
    for half, other in ((0, moved(z, nz - 1, nz)), (1, moved(z, 1, nz))):
        first = start_of(q * nz + other)
        for level in range(2):
            outgoing[half, pl.ds(2 + level, devices, stride=4), :] = near[half, level, pl.ds(first, devices), :]

    reach = nz // 2

    def hops(offset):
        i, j, side, k = offset
        return min(i, nx - i) + min(j, ny - j) / 2 + (j % 2) * 0.1 + k

    order = sorted(
        (
            (i, j, side, k)
            for i in range(nx) for j in range(ny) for side in range(2) for k in range(reach) if i or j or k
        ),
        key=lambda t: (-hops(t), t),
    )
    zs = [moved(z, k, nz) for k in range(nz)]

    def send_blocks(offsets):
        for i, j, side, k in offsets:
            px, py, tz = xs[i], ys[j], zs[(nz - k) % nz if side else k]
            target = (px * ny + py) * nz + tz
            pltpu.make_async_remote_copy(
                outgoing.at[side, pl.ds(4 * target, 4)],
                arrived.at[(side * plane + q) * reach + k],
                b_send, b_recv, device_id=(px, py, tz), device_id_type=MESH,
            ).start()

    send_blocks(order[:LATE])
    drain(fline, nz - 1, fz_recv)
    group = lax.broadcasted_iota(I32, (plane, devices), 1)
    target = lax.broadcasted_iota(I32, (plane, devices), 0) * nz + z
    picked = jnp.concatenate(
        [
            jnp.where(group == lax.rem(target + start_of(q * nz + k), devices), 1.0, 0.0).astype(BF16)
            for k in range(nz)
        ],
        axis=0,
    )
    table = jnp.concatenate(
        [fline[k] for k in range(nz)] + [jnp.zeros((128 - 4 * nz, devices), F32)], axis=0
    )
    sent = sum(
        lax.dot_general(picked, part, (((1,), (1,)), ((), ())), preferred_element_type=F32)
        for part in split3(table)
    )
    flane = lax.broadcasted_iota(I32, (devices, 128), 1)
    frow = lax.broadcasted_iota(I32, (devices, 128), 0)
    sent = jnp.where(lax.div(flane, 4) == lax.div(frow, plane), sent, 0.0)
    fsend[...] = jnp.sum(sent.reshape(nz, plane, 128), axis=0).reshape(plane, 1, 128)
    for px, py in peers:
        pltpu.make_async_remote_copy(
            fsend.at[px * ny + py], frecv.at[q], fp_send, fp_recv, device_id=(px, py, z), device_id_type=MESH
        ).start()
    send_blocks(order[LATE:])
    owns = [
        pltpu.make_async_copy(
            outgoing.at[side, pl.ds(4 * me, 4)], arrived.at[(side * plane + q) * reach], own_sems.at[side]
        )
        for side in range(2)
    ]
    for own in owns:
        own.start()

    before = lax.broadcasted_iota(I32, (devices, devices), 0) < lax.broadcasted_iota(I32, (devices, devices), 1)
    before = jnp.where(before, 1.0, 0.0).astype(BF16)
    tops = jnp.broadcast_to((counts // 8).astype(F32).astype(BF16), (8, devices))
    rests = jnp.broadcast_to((counts % 8).astype(F32).astype(BF16), (8, devices))
    offsets = (8.0 * dot(tops, before) + dot(rests, before))[0:1].astype(I32)
    places = []
    for level in range(2):
        position = level * devices + (me - offsets) % devices
        place = (offsets + position) // devices
        places.append(jnp.where(position < counts, place, -1))
    place = jnp.concatenate(places, axis=1)
    picks = jnp.where(lax.broadcasted_iota(I32, (span, span), 0) == place, 1.0, 0.0).astype(BF16)

    frecv[q] = fsend[q]
    drain(frecv, plane - 1, fp_recv)
    wide = jnp.broadcast_to(frecv[...], (plane, nz, 128)).reshape(devices, 128)
    fit = lax.div(flane, 4) == lax.rem(frow, nz)
    chosen = jnp.concatenate(
        [jnp.where(fit & (lax.rem(flane, 2) == level), wide, 0.0) for level in range(2)], axis=0
    )
    hi, mid, lo = split3(chosen)
    found = ((dot(picks, hi) + dot(picks, mid)) + dot(picks, lo)).T
    is_key = lax.rem(lax.broadcasted_iota(I32, (128, span), 0), 4) >= 2
    small[0:1] = jnp.sum(jnp.where(is_key, 0.0, found), axis=0, keepdims=True).astype(I32)
    small[1:2] = jnp.sum(jnp.where(is_key, found, 0.0), axis=0, keepdims=True).astype(I32) - 1
    level_row = lax.broadcasted_iota(I32, (8, devices), 0)
    natural = jnp.where(level_row == 0, place[:, :devices], place[:, devices:]).astype(F32) + 1.0
    hi, lo = split2(natural)
    slot = lax.broadcasted_iota(I32, (devices, devices), 1)
    holder = lax.div(lax.rem(slot, devices // 2), reach)
    shift = lax.rem(slot, reach)
    direct = slot < devices // 2
    for row, step_z in (
        (2, jnp.where(direct, nz + shift, nz - shift - 1)),
        (3, jnp.where(direct, nz - shift, nz + shift + 1)),
    ):
        source = holder * nz + lax.rem(z + step_z, nz)
        match = lax.broadcasted_iota(I32, (devices, devices), 0) == source
        match = jnp.where(match, 1.0, 0.0).astype(BF16)
        ordered = (dot(hi, match) + dot(lo, match)).astype(I32) - 1
        small[row : row + 1] = jnp.concatenate([ordered[0:1], ordered[1:2]], axis=1)
    small[4:5] = jnp.broadcast_to(jnp.sum(counts, axis=1, keepdims=True), (1, span))
    for own in owns:
        own.wait()
    drain(arrived, devices - 2, b_recv)
    drain(cline, nz - 1, cz_send)
    drain(call, plane - 1, cp_send)
    drain(fsend, plane - 1, fp_send)
    drain(fline, nz - 1, fz_send)
    drain(arrived, devices - 2, b_send)
    pltpu.make_async_copy(acc, acc, near_send).wait()


def put(arrived, small, out_sums, out_rows, out_keys, out_total):
    span = out_sums.shape[0]
    senders = span // 2
    slots = senders // 2
    out_rows[...] = small[0:1]
    out_keys[...] = small[1:2]
    out_total[...] = small[4:5, 0:1]
    labels = lax.broadcasted_iota(I32, (span, senders), 0)
    sides = []
    for half in range(2):
        direct, relayed = (4 * slots, 2) if half == 0 else (0, 4 * slots + 2)
        total = None
        for level in range(2):
            block = jnp.concatenate(
                [arrived[pl.ds(base + level, slots, stride=4), :] for base in (direct, relayed)], axis=0
            )
            places = small[2 + half : 3 + half, level * senders : (level + 1) * senders]
            picks = jnp.where(labels == places, 1.0, 0.0).astype(BF16)
            part = dot(picks, jnp.concatenate(split2(block), axis=1))
            total = part if total is None else total + part
        sides.append(total[:, :128] + total[:, 128:])
    out_sums[...] = jnp.concatenate(sides, axis=1)


def solution(mesh):
    sizes = tuple(mesh.shape[a] for a in AXES)
    nx, ny, nz = sizes
    plane, devices = nx * ny, nx * ny * nz
    vmem = pl.BlockSpec(memory_space=pltpu.VMEM)

    def shards(measures, group_index, distinct_keys, group_counts):
        rows, width = measures.shape
        span = distinct_keys.shape[1]
        hbm = pl.BlockSpec(memory_space=pl.ANY)
        arrived, small = pl.pallas_call(
            functools.partial(kernel, sizes),
            out_shape=(
                jax.ShapeDtypeStruct((devices, 4, 128), F32),
                jax.ShapeDtypeStruct((8, span), I32),
            ),
            in_specs=[hbm] * 3,
            out_specs=(pl.BlockSpec(memory_space=pl.ANY), vmem),
            scratch_shapes=[
                pltpu.VMEM((rows, width), F32),
                pltpu.VMEM((1, rows), I32),
                pltpu.VMEM((1, span), I32),
                pltpu.VMEM((span, width), F32),
                pltpu.VMEM((span, 128), F32),
                pltpu.VMEM((2, 2, span, 128), F32),
                pltpu.VMEM((2, 2, span, 128), F32),
                pltpu.VMEM((2, 4 * devices, 128), F32),
                pltpu.VMEM((plane, 1, 128), F32),
                pltpu.VMEM((plane, 1, 128), F32),
                pltpu.VMEM((1, 4, devices), F32),
                pltpu.VMEM((nz, 4, devices), F32),
                pltpu.VMEM((1, 1, 128), I32),
                pltpu.VMEM((nz, 1, 128), I32),
                pltpu.VMEM((1, 1, 128), I32),
                pltpu.VMEM((plane, 1, 128), I32),
                pltpu.SemaphoreType.DMA((CHUNKS + 2,)),
                pltpu.SemaphoreType.DMA((2,)),
            ]
            + [pltpu.SemaphoreType.DMA(())] * 12,
            compiler_params=pltpu.CompilerParams(
                collective_id=0, has_side_effects=True, vmem_limit_bytes=32 << 20
            ),
            name="exchange",
        )(*(
            pltpu.with_memory_space_constraint(a, pltpu.MemorySpace.HBM)
            for a in (measures, group_index.reshape(1, rows), distinct_keys)
        ))
        sums, tallies, keys, total = pl.pallas_call(
            put,
            out_shape=(
                jax.ShapeDtypeStruct((span, width), F32),
                jax.ShapeDtypeStruct((1, span), I32),
                jax.ShapeDtypeStruct((1, span), I32),
                jax.ShapeDtypeStruct((1, 1), I32),
            ),
            in_specs=[vmem] * 2,
            out_specs=(vmem,) * 4,
            compiler_params=pltpu.CompilerParams(vmem_limit_bytes=24 << 20),
            name="put",
        )(arrived.reshape(4 * devices, 128), small)
        return sums, tallies.reshape(span), keys.reshape(span), total.reshape(())

    return jax.shard_map(
        shards,
        mesh=mesh,
        in_specs=(P(AXES, None), P(AXES), P(AXES, None), P(AXES)),
        out_specs=(P(AXES, None), P(AXES), P(AXES), P()),
        check_vma=False,
    )
```

```python
import functools

import jax
import jax.numpy as jnp
from jax import lax
from jax.experimental import pallas as pl
from jax.experimental.pallas import tpu as pltpu
from jax.sharding import PartitionSpec as P

AXES = ("gx", "gy", "gz")
MESH = pl.DeviceIdType.MESH
F32, BF16, I32 = jnp.float32, jnp.bfloat16, jnp.int32
CHUNKS = 4
LATE = 150


def split2(v):
    hi = v.astype(BF16)
    lo = (v - hi.astype(F32)).astype(BF16)
    return hi, lo


def split3(v):
    hi = v.astype(BF16)
    rest = v - hi.astype(F32)
    mid = rest.astype(BF16)
    lo = (rest - mid.astype(F32)).astype(BF16)
    return hi, mid, lo


def dot(a, b):
    return jnp.dot(a, b, preferred_element_type=F32)


def kernel(
    sizes,
    measures, index_in, keys_in,
    arrived, small,
    values, index, keys, acc, tally, halves, near, outgoing, fsend, frecv, fown, fline,
    crow, cline, crelay, call,
    load_sems, own_sems, near_send, near_recv, cz_send, cz_recv, cp_send, cp_recv, fp_send, fp_recv, fz_send, fz_recv, b_send, b_recv,
):
    nx, ny, nz = sizes
    plane, devices = nx * ny, nx * ny * nz
    rows = measures.shape[0]
    step = rows // CHUNKS
    span = 2 * devices
    x, y, z = (lax.axis_index(a) for a in AXES)
    q = x * ny + y
    me = q * nz + z

    def outward(n):
        return sorted(range(n), key=lambda k: -min(k, n - k))

    def moved(base, k, n):
        return lax.rem(base + k, n) if k else base

    lines = [(k, moved(z, k, nz)) for k in outward(nz) if k]
    across = sorted(
        ((i, j) for i in range(nx) for j in range(ny) if i or j),
        key=lambda t: -(min(t[0], nx - t[0]) + min(t[1], ny - t[1]) / 2),
    )
    xs = [moved(x, k, nx) for k in range(nx)]
    ys = [moved(y, k, ny) for k in range(ny)]
    peers = [(xs[i], ys[j]) for i, j in across]

    barrier = pltpu.get_barrier_semaphore()
    for px, py in peers:
        pl.semaphore_signal(barrier, inc=1, device_id=(px, py, z), device_id_type=MESH)
    for _, tz in lines:
        pl.semaphore_signal(barrier, inc=1, device_id=(x, y, tz), device_id_type=MESH)

    loads = [
        pltpu.make_async_copy(
            measures.at[pl.ds(c * step, step)], values.at[pl.ds(c * step, step)], load_sems.at[c]
        )
        for c in range(CHUNKS)
    ]
    inputs = [
        pltpu.make_async_copy(src, dst, load_sems.at[CHUNKS + i])
        for i, (src, dst) in enumerate(((index_in, index), (keys_in, keys)))
    ]
    for load in inputs + loads:
        load.start()

    for load in inputs:
        load.wait()
    count = jnp.max(index[...], axis=1, keepdims=True) + 1
    lane = lax.broadcasted_iota(I32, (1, 128), 1)
    mine = jnp.where(lane == me % 128, count, 0)
    crow[0] = mine
    cline[z] = mine

    labels = lax.broadcasted_iota(I32, (span, step), 0)

    ones = jnp.ones((step, 128), BF16)

    def accumulate(c):
        loads[c].wait()
        hits = jnp.where(labels == index[0:1, c * step : (c + 1) * step], 1.0, 0.0).astype(BF16)
        hi, lo = split2(values[pl.ds(c * step, step)])
        part = dot(hits, hi) + dot(hits, lo)
        seen = dot(hits, ones)
        if c == 0:
            acc[...] = part
            tally[...] = seen
        else:
            acc[...] += part
            tally[...] += seen

    for c in range(CHUNKS // 2):
        accumulate(c)
    pl.semaphore_wait(barrier, nz - 1 + plane - 1)

    for _, tz in lines:
        pltpu.make_async_remote_copy(
            crow.at[0], cline.at[z], cz_send, cz_recv, device_id=(x, y, tz), device_id_type=MESH
        ).start()
    for c in range(CHUNKS // 2, CHUNKS):
        accumulate(c)

    def drain(ref, n, sem):
        pltpu.make_async_copy(ref.at[pl.ds(0, n)], ref.at[pl.ds(0, n)], sem).wait()

    for half in range(2):
        for level in range(2):
            part = acc[pl.ds(level * devices, devices), pl.ds(half * 128, 128)]
            halves[half, level, pl.ds(0, devices), :] = part
            halves[half, level, pl.ds(devices, devices), :] = part
    for half, tz in ((0, moved(z, 1, nz)), (1, moved(z, nz - 1, nz))):
        for level in range(2):
            pltpu.make_async_remote_copy(
                halves.at[half, level, pl.ds(0, devices)], near.at[half, level, pl.ds(0, devices)],
                near_send, near_recv, device_id=(x, y, tz), device_id_type=MESH,
            ).start()
    seen = tally[...].T[0:1]
    named = keys[...].astype(F32) + 1.0
    fown[0] = jnp.concatenate(
        [row[:, level * devices : (level + 1) * devices] for row in (seen, named) for level in range(2)], axis=0
    )
    fline[z] = fown[0]
    for _, tz in lines:
        pltpu.make_async_remote_copy(
            fown.at[0], fline.at[z], fz_send, fz_recv, device_id=(x, y, tz), device_id_type=MESH
        ).start()
    drain(cline, nz - 1, cz_recv)
    relayed = cline[0]
    for k in range(1, nz):
        relayed = relayed + cline[k]
    crelay[0] = relayed
    call[q] = relayed

    for px, py in peers:
        pltpu.make_async_remote_copy(
            crelay.at[0], call.at[q], cp_send, cp_recv, device_id=(px, py, z), device_id_type=MESH
        ).start()

    pltpu.make_async_copy(acc, acc, near_recv).wait()
    for half in range(2):
        for level in range(2):
            near[half, level, pl.ds(devices, devices), :] = near[half, level, pl.ds(0, devices), :]
    drain(call, plane - 1, cp_recv)
    low = jnp.sum(call[pl.ds(0, plane // 2)], axis=0)
    high = jnp.sum(call[pl.ds(plane // 2, plane // 2)], axis=0)
    counts = jnp.concatenate([low, high], axis=1)
    lanes = lax.broadcasted_iota(I32, (1, devices), 1)

    def start_of(device):
        return devices - lax.rem(jnp.sum(jnp.where(lanes < device, counts, 0)), devices)

    start = start_of(me)
    for level in range(2):
        outgoing[0, pl.ds(level, devices, stride=4), :] = halves[1, level, pl.ds(start, devices), :]
        outgoing[1, pl.ds(level, devices, stride=4), :] = halves[0, level, pl.ds(start, devices), :]
    for half, other in ((0, moved(z, nz - 1, nz)), (1, moved(z, 1, nz))):
        first = start_of(q * nz + other)
        for level in range(2):
            outgoing[half, pl.ds(2 + level, devices, stride=4), :] = near[half, level, pl.ds(first, devices), :]

    reach = nz // 2

    def hops(offset):
        i, j, side, k = offset
        return 2 * (min(i, nx - i) + min(j, ny - j) / 2 + (j % 2) * 0.1) + k

    order = sorted(
        (
            (i, j, side, k)
            for i in range(nx) for j in range(ny) for side in range(2) for k in range(reach) if i or j or k
        ),
        key=lambda t: (-hops(t), t),
    )
    zs = [moved(z, k, nz) for k in range(nz)]

    def send_blocks(offsets):
        for i, j, side, k in offsets:
            px, py, tz = xs[i], ys[j], zs[(nz - k) % nz if side else k]
            target = (px * ny + py) * nz + tz
            pltpu.make_async_remote_copy(
                outgoing.at[side, pl.ds(4 * target, 4)],
                arrived.at[(side * plane + q) * reach + k],
                b_send, b_recv, device_id=(px, py, tz), device_id_type=MESH,
            ).start()

    send_blocks(order[:LATE])
    drain(fline, nz - 1, fz_recv)
    group = lax.broadcasted_iota(I32, (plane, devices), 1)
    target = lax.broadcasted_iota(I32, (plane, devices), 0) * nz + z
    picked = jnp.concatenate(
        [
            jnp.where(group == lax.rem(target + start_of(q * nz + k), devices), 1.0, 0.0).astype(BF16)
            for k in range(nz)
        ],
        axis=0,
    )
    table = jnp.concatenate(
        [fline[k] for k in range(nz)] + [jnp.zeros((128 - 4 * nz, devices), F32)], axis=0
    )
    sent = sum(
        lax.dot_general(picked, part, (((1,), (1,)), ((), ())), preferred_element_type=F32)
        for part in split3(table)
    )
    flane = lax.broadcasted_iota(I32, (devices, 128), 1)
    frow = lax.broadcasted_iota(I32, (devices, 128), 0)
    sent = jnp.where(lax.div(flane, 4) == lax.div(frow, plane), sent, 0.0)
    fsend[...] = jnp.sum(sent.reshape(nz, plane, 128), axis=0).reshape(plane, 1, 128)
    for px, py in peers:
        pltpu.make_async_remote_copy(
            fsend.at[px * ny + py], frecv.at[q], fp_send, fp_recv, device_id=(px, py, z), device_id_type=MESH
        ).start()
    send_blocks(order[LATE:])
    owns = [
        pltpu.make_async_copy(
            outgoing.at[side, pl.ds(4 * me, 4)], arrived.at[(side * plane + q) * reach], own_sems.at[side]
        )
        for side in range(2)
    ]
    for own in owns:
        own.start()

    before = lax.broadcasted_iota(I32, (devices, devices), 0) < lax.broadcasted_iota(I32, (devices, devices), 1)
    before = jnp.where(before, 1.0, 0.0).astype(BF16)
    tops = jnp.broadcast_to((counts // 8).astype(F32).astype(BF16), (8, devices))
    rests = jnp.broadcast_to((counts % 8).astype(F32).astype(BF16), (8, devices))
    offsets = (8.0 * dot(tops, before) + dot(rests, before))[0:1].astype(I32)
    places = []
    for level in range(2):
        position = level * devices + (me - offsets) % devices
        place = (offsets + position) // devices
        places.append(jnp.where(position < counts, place, -1))
    place = jnp.concatenate(places, axis=1)
    picks = jnp.where(lax.broadcasted_iota(I32, (span, span), 0) == place, 1.0, 0.0).astype(BF16)

    frecv[q] = fsend[q]
    drain(frecv, plane - 1, fp_recv)
    wide = jnp.broadcast_to(frecv[...], (plane, nz, 128)).reshape(devices, 128)
    fit = lax.div(flane, 4) == lax.rem(frow, nz)
    chosen = jnp.concatenate(
        [jnp.where(fit & (lax.rem(flane, 2) == level), wide, 0.0) for level in range(2)], axis=0
    )
    hi, mid, lo = split3(chosen)
    found = ((dot(picks, hi) + dot(picks, mid)) + dot(picks, lo)).T
    is_key = lax.rem(lax.broadcasted_iota(I32, (128, span), 0), 4) >= 2
    small[0:1] = jnp.sum(jnp.where(is_key, 0.0, found), axis=0, keepdims=True).astype(I32)
    small[1:2] = jnp.sum(jnp.where(is_key, found, 0.0), axis=0, keepdims=True).astype(I32) - 1
    level_row = lax.broadcasted_iota(I32, (8, devices), 0)
    natural = jnp.where(level_row == 0, place[:, :devices], place[:, devices:]).astype(F32) + 1.0
    hi, lo = split2(natural)
    slot = lax.broadcasted_iota(I32, (devices, devices), 1)
    holder = lax.div(lax.rem(slot, devices // 2), reach)
    shift = lax.rem(slot, reach)
    direct = slot < devices // 2
    for row, step_z in (
        (2, jnp.where(direct, nz + shift, nz - shift - 1)),
        (3, jnp.where(direct, nz - shift, nz + shift + 1)),
    ):
        source = holder * nz + lax.rem(z + step_z, nz)
        match = lax.broadcasted_iota(I32, (devices, devices), 0) == source
        match = jnp.where(match, 1.0, 0.0).astype(BF16)
        ordered = (dot(hi, match) + dot(lo, match)).astype(I32) - 1
        small[row : row + 1] = jnp.concatenate([ordered[0:1], ordered[1:2]], axis=1)
    small[4:5] = jnp.broadcast_to(jnp.sum(counts, axis=1, keepdims=True), (1, span))
    for own in owns:
        own.wait()
    drain(arrived, devices - 2, b_recv)
    drain(cline, nz - 1, cz_send)
    drain(call, plane - 1, cp_send)
    drain(fsend, plane - 1, fp_send)
    drain(fline, nz - 1, fz_send)
    drain(arrived, devices - 2, b_send)
    pltpu.make_async_copy(acc, acc, near_send).wait()


def put(arrived, small, out_sums, out_rows, out_keys, out_total):
    span = out_sums.shape[0]
    senders = span // 2
    slots = senders // 2
    out_rows[...] = small[0:1]
    out_keys[...] = small[1:2]
    out_total[...] = small[4:5, 0:1]
    labels = lax.broadcasted_iota(I32, (span, senders), 0)
    sides = []
    for half in range(2):
        direct, relayed = (4 * slots, 2) if half == 0 else (0, 4 * slots + 2)
        total = None
        for level in range(2):
            block = jnp.concatenate(
                [arrived[pl.ds(base + level, slots, stride=4), :] for base in (direct, relayed)], axis=0
            )
            places = small[2 + half : 3 + half, level * senders : (level + 1) * senders]
            picks = jnp.where(labels == places, 1.0, 0.0).astype(BF16)
            part = dot(picks, jnp.concatenate(split2(block), axis=1))
            total = part if total is None else total + part
        sides.append(total[:, :128] + total[:, 128:])
    out_sums[...] = jnp.concatenate(sides, axis=1)


def solution(mesh):
    sizes = tuple(mesh.shape[a] for a in AXES)
    nx, ny, nz = sizes
    plane, devices = nx * ny, nx * ny * nz
    vmem = pl.BlockSpec(memory_space=pltpu.VMEM)

    def shards(measures, group_index, distinct_keys, group_counts):
        rows, width = measures.shape
        span = distinct_keys.shape[1]
        hbm = pl.BlockSpec(memory_space=pl.ANY)
        arrived, small = pl.pallas_call(
            functools.partial(kernel, sizes),
            out_shape=(
                jax.ShapeDtypeStruct((devices, 4, 128), F32),
                jax.ShapeDtypeStruct((8, span), I32),
            ),
            in_specs=[hbm] * 3,
            out_specs=(pl.BlockSpec(memory_space=pl.ANY), vmem),
            scratch_shapes=[
                pltpu.VMEM((rows, width), F32),
                pltpu.VMEM((1, rows), I32),
                pltpu.VMEM((1, span), I32),
                pltpu.VMEM((span, width), F32),
                pltpu.VMEM((span, 128), F32),
                pltpu.VMEM((2, 2, span, 128), F32),
                pltpu.VMEM((2, 2, span, 128), F32),
                pltpu.VMEM((2, 4 * devices, 128), F32),
                pltpu.VMEM((plane, 1, 128), F32),
                pltpu.VMEM((plane, 1, 128), F32),
                pltpu.VMEM((1, 4, devices), F32),
                pltpu.VMEM((nz, 4, devices), F32),
                pltpu.VMEM((1, 1, 128), I32),
                pltpu.VMEM((nz, 1, 128), I32),
                pltpu.VMEM((1, 1, 128), I32),
                pltpu.VMEM((plane, 1, 128), I32),
                pltpu.SemaphoreType.DMA((CHUNKS + 2,)),
                pltpu.SemaphoreType.DMA((2,)),
            ]
            + [pltpu.SemaphoreType.DMA(())] * 12,
            compiler_params=pltpu.CompilerParams(
                collective_id=0, has_side_effects=True, vmem_limit_bytes=32 << 20
            ),
            name="exchange",
        )(*(
            pltpu.with_memory_space_constraint(a, pltpu.MemorySpace.HBM)
            for a in (measures, group_index.reshape(1, rows), distinct_keys)
        ))
        sums, tallies, keys, total = pl.pallas_call(
            put,
            out_shape=(
                jax.ShapeDtypeStruct((span, width), F32),
                jax.ShapeDtypeStruct((1, span), I32),
                jax.ShapeDtypeStruct((1, span), I32),
                jax.ShapeDtypeStruct((1, 1), I32),
            ),
            in_specs=[vmem] * 2,
            out_specs=(vmem,) * 4,
            compiler_params=pltpu.CompilerParams(vmem_limit_bytes=24 << 20),
            name="put",
        )(arrived.reshape(4 * devices, 128), small)
        return sums, tallies.reshape(span), keys.reshape(span), total.reshape(())

    return jax.shard_map(
        shards,
        mesh=mesh,
        in_specs=(P(AXES, None), P(AXES), P(AXES, None), P(AXES)),
        out_specs=(P(AXES, None), P(AXES), P(AXES), P()),
        check_vma=False,
    )
```

```python
import functools

import jax
import jax.numpy as jnp
from jax import lax
from jax.experimental import pallas as pl
from jax.experimental.pallas import tpu as pltpu
from jax.sharding import PartitionSpec as P

AXES = ("gx", "gy", "gz")
MESH = pl.DeviceIdType.MESH
F32, BF16, I32 = jnp.float32, jnp.bfloat16, jnp.int32
CHUNKS = 2
LATE = 150


def split2(v):
    hi = v.astype(BF16)
    lo = (v - hi.astype(F32)).astype(BF16)
    return hi, lo


def split3(v):
    hi = v.astype(BF16)
    rest = v - hi.astype(F32)
    mid = rest.astype(BF16)
    lo = (rest - mid.astype(F32)).astype(BF16)
    return hi, mid, lo


def dot(a, b):
    return jnp.dot(a, b, preferred_element_type=F32)


def kernel(
    sizes,
    measures, index_in, keys_in,
    arrived, small,
    values, index, keys, acc, tally, halves, near, outgoing, fsend, frecv, fown, fline,
    crow, cline, crelay, call,
    load_sems, own_sems, near_send, near_recv, cz_send, cz_recv, cp_send, cp_recv, fp_send, fp_recv, fz_send, fz_recv, b_send, b_recv,
):
    nx, ny, nz = sizes
    plane, devices = nx * ny, nx * ny * nz
    rows = measures.shape[0]
    step = rows // CHUNKS
    span = 2 * devices
    x, y, z = (lax.axis_index(a) for a in AXES)
    q = x * ny + y
    me = q * nz + z

    def outward(n):
        return sorted(range(n), key=lambda k: -min(k, n - k))

    def moved(base, k, n):
        return lax.rem(base + k, n) if k else base

    lines = [(k, moved(z, k, nz)) for k in outward(nz) if k]
    across = sorted(
        ((i, j) for i in range(nx) for j in range(ny) if i or j),
        key=lambda t: -(min(t[0], nx - t[0]) + min(t[1], ny - t[1]) / 2),
    )
    xs = [moved(x, k, nx) for k in range(nx)]
    ys = [moved(y, k, ny) for k in range(ny)]
    peers = [(xs[i], ys[j]) for i, j in across]

    barrier = pltpu.get_barrier_semaphore()
    greeted = [(min(i, nx - i) + min(j, ny - j) / 2, (px, py, z)) for (i, j), (px, py) in zip(across, peers)]
    greeted += [(min(k, nz - k), (x, y, tz)) for k, tz in lines]
    for _, place in sorted(greeted, key=lambda t: -t[0]):
        pl.semaphore_signal(barrier, inc=1, device_id=place, device_id_type=MESH)

    loads = [
        pltpu.make_async_copy(
            measures.at[pl.ds(c * step, step)], values.at[pl.ds(c * step, step)], load_sems.at[c]
        )
        for c in range(CHUNKS)
    ]
    inputs = [
        pltpu.make_async_copy(src, dst, load_sems.at[CHUNKS + i])
        for i, (src, dst) in enumerate(((index_in, index), (keys_in, keys)))
    ]
    for load in inputs + loads:
        load.start()

    for load in inputs:
        load.wait()
    count = jnp.max(index[...], axis=1, keepdims=True) + 1
    lane = lax.broadcasted_iota(I32, (1, 128), 1)
    mine = jnp.where(lane == me % 128, count, 0)
    crow[0] = mine
    cline[z] = mine

    labels = lax.broadcasted_iota(I32, (span, step), 0)

    ones = jnp.ones((step, 128), BF16)

    def accumulate(c):
        loads[c].wait()
        hits = jnp.where(labels == index[0:1, c * step : (c + 1) * step], 1.0, 0.0).astype(BF16)
        hi, lo = split2(values[pl.ds(c * step, step)])
        part = dot(hits, hi) + dot(hits, lo)
        seen = dot(hits, ones)
        if c == 0:
            acc[...] = part
            tally[...] = seen
        else:
            acc[...] += part
            tally[...] += seen

    for c in range(CHUNKS // 2):
        accumulate(c)
    pl.semaphore_wait(barrier, nz - 1 + plane - 1)

    for _, tz in lines:
        pltpu.make_async_remote_copy(
            crow.at[0], cline.at[z], cz_send, cz_recv, device_id=(x, y, tz), device_id_type=MESH
        ).start()
    for c in range(CHUNKS // 2, CHUNKS):
        accumulate(c)

    def drain(ref, n, sem):
        pltpu.make_async_copy(ref.at[pl.ds(0, n)], ref.at[pl.ds(0, n)], sem).wait()

    for half in range(2):
        for level in range(2):
            part = acc[pl.ds(level * devices, devices), pl.ds(half * 128, 128)]
            halves[half, level, pl.ds(0, devices), :] = part
            halves[half, level, pl.ds(devices, devices), :] = part
    for half, tz in ((0, moved(z, 1, nz)), (1, moved(z, nz - 1, nz))):
        for level in range(2):
            pltpu.make_async_remote_copy(
                halves.at[half, level, pl.ds(0, devices)], near.at[half, level, pl.ds(0, devices)],
                near_send, near_recv, device_id=(x, y, tz), device_id_type=MESH,
            ).start()
    seen = tally[...].T[0:1]
    named = keys[...].astype(F32) + 1.0
    fown[0] = jnp.concatenate(
        [row[:, level * devices : (level + 1) * devices] for row in (seen, named) for level in range(2)], axis=0
    )
    fline[z] = fown[0]
    for _, tz in lines:
        pltpu.make_async_remote_copy(
            fown.at[0], fline.at[z], fz_send, fz_recv, device_id=(x, y, tz), device_id_type=MESH
        ).start()
    drain(cline, nz - 1, cz_recv)
    relayed = cline[0]
    for k in range(1, nz):
        relayed = relayed + cline[k]
    crelay[0] = relayed
    call[q] = relayed

    for px, py in peers:
        pltpu.make_async_remote_copy(
            crelay.at[0], call.at[q], cp_send, cp_recv, device_id=(px, py, z), device_id_type=MESH
        ).start()

    pltpu.make_async_copy(acc, acc, near_recv).wait()
    for half in range(2):
        for level in range(2):
            near[half, level, pl.ds(devices, devices), :] = near[half, level, pl.ds(0, devices), :]
    drain(call, plane - 1, cp_recv)
    low = jnp.sum(call[pl.ds(0, plane // 2)], axis=0)
    high = jnp.sum(call[pl.ds(plane // 2, plane // 2)], axis=0)
    counts = jnp.concatenate([low, high], axis=1)
    lanes = lax.broadcasted_iota(I32, (1, devices), 1)

    def start_of(device):
        return devices - lax.rem(jnp.sum(jnp.where(lanes < device, counts, 0)), devices)

    start = start_of(me)
    for level in range(2):
        outgoing[0, pl.ds(level, devices, stride=4), :] = halves[1, level, pl.ds(start, devices), :]
        outgoing[1, pl.ds(level, devices, stride=4), :] = halves[0, level, pl.ds(start, devices), :]
    for half, other in ((0, moved(z, nz - 1, nz)), (1, moved(z, 1, nz))):
        first = start_of(q * nz + other)
        for level in range(2):
            outgoing[half, pl.ds(2 + level, devices, stride=4), :] = near[half, level, pl.ds(first, devices), :]

    reach = nz // 2

    def hops(offset):
        i, j, side, k = offset
        return 2 * (min(i, nx - i) + min(j, ny - j) / 2 + (j % 2) * 0.1) + k

    order = sorted(
        (
            (i, j, side, k)
            for i in range(nx) for j in range(ny) for side in range(2) for k in range(reach) if i or j or k
        ),
        key=lambda t: (-hops(t), t),
    )
    zs = [moved(z, k, nz) for k in range(nz)]

    def send_blocks(offsets):
        for i, j, side, k in offsets:
            px, py, tz = xs[i], ys[j], zs[(nz - k) % nz if side else k]
            target = (px * ny + py) * nz + tz
            pltpu.make_async_remote_copy(
                outgoing.at[side, pl.ds(4 * target, 4)],
                arrived.at[(side * plane + q) * reach + k],
                b_send, b_recv, device_id=(px, py, tz), device_id_type=MESH,
            ).start()

    send_blocks(order[:LATE])
    drain(fline, nz - 1, fz_recv)
    group = lax.broadcasted_iota(I32, (plane, devices), 1)
    target = lax.broadcasted_iota(I32, (plane, devices), 0) * nz + z
    picked = jnp.concatenate(
        [
            jnp.where(group == lax.rem(target + start_of(q * nz + k), devices), 1.0, 0.0).astype(BF16)
            for k in range(nz)
        ],
        axis=0,
    )
    table = jnp.concatenate(
        [fline[k] for k in range(nz)] + [jnp.zeros((128 - 4 * nz, devices), F32)], axis=0
    )
    sent = sum(
        lax.dot_general(picked, part, (((1,), (1,)), ((), ())), preferred_element_type=F32)
        for part in split3(table)
    )
    flane = lax.broadcasted_iota(I32, (devices, 128), 1)
    frow = lax.broadcasted_iota(I32, (devices, 128), 0)
    sent = jnp.where(lax.div(flane, 4) == lax.div(frow, plane), sent, 0.0)
    fsend[...] = jnp.sum(sent.reshape(nz, plane, 128), axis=0).reshape(plane, 1, 128)
    for px, py in peers:
        pltpu.make_async_remote_copy(
            fsend.at[px * ny + py], frecv.at[q], fp_send, fp_recv, device_id=(px, py, z), device_id_type=MESH
        ).start()
    send_blocks(order[LATE:])
    owns = [
        pltpu.make_async_copy(
            outgoing.at[side, pl.ds(4 * me, 4)], arrived.at[(side * plane + q) * reach], own_sems.at[side]
        )
        for side in range(2)
    ]
    for own in owns:
        own.start()

    before = lax.broadcasted_iota(I32, (devices, devices), 0) < lax.broadcasted_iota(I32, (devices, devices), 1)
    before = jnp.where(before, 1.0, 0.0).astype(BF16)
    tops = jnp.broadcast_to((counts // 8).astype(F32).astype(BF16), (8, devices))
    rests = jnp.broadcast_to((counts % 8).astype(F32).astype(BF16), (8, devices))
    offsets = (8.0 * dot(tops, before) + dot(rests, before))[0:1].astype(I32)
    places = []
    for level in range(2):
        position = level * devices + (me - offsets) % devices
        place = (offsets + position) // devices
        places.append(jnp.where(position < counts, place, -1))
    place = jnp.concatenate(places, axis=1)
    picks = jnp.where(lax.broadcasted_iota(I32, (span, span), 0) == place, 1.0, 0.0).astype(BF16)

    frecv[q] = fsend[q]
    drain(frecv, plane - 1, fp_recv)
    wide = jnp.broadcast_to(frecv[...], (plane, nz, 128)).reshape(devices, 128)
    fit = lax.div(flane, 4) == lax.rem(frow, nz)
    chosen = jnp.concatenate(
        [jnp.where(fit & (lax.rem(flane, 2) == level), wide, 0.0) for level in range(2)], axis=0
    )
    hi, mid, lo = split3(chosen)
    found = ((dot(picks, hi) + dot(picks, mid)) + dot(picks, lo)).T
    is_key = lax.rem(lax.broadcasted_iota(I32, (128, span), 0), 4) >= 2
    small[0:1] = jnp.sum(jnp.where(is_key, 0.0, found), axis=0, keepdims=True).astype(I32)
    small[1:2] = jnp.sum(jnp.where(is_key, found, 0.0), axis=0, keepdims=True).astype(I32) - 1
    level_row = lax.broadcasted_iota(I32, (8, devices), 0)
    natural = jnp.where(level_row == 0, place[:, :devices], place[:, devices:]).astype(F32) + 1.0
    hi, lo = split2(natural)
    slot = lax.broadcasted_iota(I32, (devices, devices), 1)
    holder = lax.div(lax.rem(slot, devices // 2), reach)
    shift = lax.rem(slot, reach)
    direct = slot < devices // 2
    for row, step_z in (
        (2, jnp.where(direct, nz + shift, nz - shift - 1)),
        (3, jnp.where(direct, nz - shift, nz + shift + 1)),
    ):
        source = holder * nz + lax.rem(z + step_z, nz)
        match = lax.broadcasted_iota(I32, (devices, devices), 0) == source
        match = jnp.where(match, 1.0, 0.0).astype(BF16)
        ordered = (dot(hi, match) + dot(lo, match)).astype(I32) - 1
        small[row : row + 1] = jnp.concatenate([ordered[0:1], ordered[1:2]], axis=1)
    small[4:5] = jnp.broadcast_to(jnp.sum(counts, axis=1, keepdims=True), (1, span))
    for own in owns:
        own.wait()
    drain(arrived, devices - 2, b_recv)
    drain(cline, nz - 1, cz_send)
    drain(call, plane - 1, cp_send)
    drain(fsend, plane - 1, fp_send)
    drain(fline, nz - 1, fz_send)
    drain(arrived, devices - 2, b_send)
    pltpu.make_async_copy(acc, acc, near_send).wait()


def put(arrived, small, out_sums, out_rows, out_keys, out_total):
    span = out_sums.shape[0]
    senders = span // 2
    slots = senders // 2
    out_rows[...] = small[0:1]
    out_keys[...] = small[1:2]
    out_total[...] = small[4:5, 0:1]
    labels = lax.broadcasted_iota(I32, (span, senders), 0)
    sides = []
    for half in range(2):
        direct, relayed = (4 * slots, 2) if half == 0 else (0, 4 * slots + 2)
        total = None
        for level in range(2):
            block = jnp.concatenate(
                [arrived[pl.ds(base + level, slots, stride=4), :] for base in (direct, relayed)], axis=0
            )
            places = small[2 + half : 3 + half, level * senders : (level + 1) * senders]
            picks = jnp.where(labels == places, 1.0, 0.0).astype(BF16)
            part = dot(picks, jnp.concatenate(split2(block), axis=1))
            total = part if total is None else total + part
        sides.append(total[:, :128] + total[:, 128:])
    out_sums[...] = jnp.concatenate(sides, axis=1)


def solution(mesh):
    sizes = tuple(mesh.shape[a] for a in AXES)
    nx, ny, nz = sizes
    plane, devices = nx * ny, nx * ny * nz
    vmem = pl.BlockSpec(memory_space=pltpu.VMEM)

    def shards(measures, group_index, distinct_keys, group_counts):
        rows, width = measures.shape
        span = distinct_keys.shape[1]
        hbm = pl.BlockSpec(memory_space=pl.ANY)
        arrived, small = pl.pallas_call(
            functools.partial(kernel, sizes),
            out_shape=(
                jax.ShapeDtypeStruct((devices, 4, 128), F32),
                jax.ShapeDtypeStruct((8, span), I32),
            ),
            in_specs=[hbm] * 3,
            out_specs=(pl.BlockSpec(memory_space=pl.ANY), vmem),
            scratch_shapes=[
                pltpu.VMEM((rows, width), F32),
                pltpu.VMEM((1, rows), I32),
                pltpu.VMEM((1, span), I32),
                pltpu.VMEM((span, width), F32),
                pltpu.VMEM((span, 128), F32),
                pltpu.VMEM((2, 2, span, 128), F32),
                pltpu.VMEM((2, 2, span, 128), F32),
                pltpu.VMEM((2, 4 * devices, 128), F32),
                pltpu.VMEM((plane, 1, 128), F32),
                pltpu.VMEM((plane, 1, 128), F32),
                pltpu.VMEM((1, 4, devices), F32),
                pltpu.VMEM((nz, 4, devices), F32),
                pltpu.VMEM((1, 1, 128), I32),
                pltpu.VMEM((nz, 1, 128), I32),
                pltpu.VMEM((1, 1, 128), I32),
                pltpu.VMEM((plane, 1, 128), I32),
                pltpu.SemaphoreType.DMA((CHUNKS + 2,)),
                pltpu.SemaphoreType.DMA((2,)),
            ]
            + [pltpu.SemaphoreType.DMA(())] * 12,
            compiler_params=pltpu.CompilerParams(
                collective_id=0, has_side_effects=True, vmem_limit_bytes=32 << 20
            ),
            name="exchange",
        )(*(
            pltpu.with_memory_space_constraint(a, pltpu.MemorySpace.HBM)
            for a in (measures, group_index.reshape(1, rows), distinct_keys)
        ))
        sums, tallies, keys, total = pl.pallas_call(
            put,
            out_shape=(
                jax.ShapeDtypeStruct((span, width), F32),
                jax.ShapeDtypeStruct((1, span), I32),
                jax.ShapeDtypeStruct((1, span), I32),
                jax.ShapeDtypeStruct((1, 1), I32),
            ),
            in_specs=[vmem] * 2,
            out_specs=(vmem,) * 4,
            compiler_params=pltpu.CompilerParams(vmem_limit_bytes=24 << 20),
            name="put",
        )(arrived.reshape(4 * devices, 128), small)
        return sums, tallies.reshape(span), keys.reshape(span), total.reshape(())

    return jax.shard_map(
        shards,
        mesh=mesh,
        in_specs=(P(AXES, None), P(AXES), P(AXES, None), P(AXES)),
        out_specs=(P(AXES, None), P(AXES), P(AXES), P()),
        check_vma=False,
    )
```

```python
import functools

import jax
import jax.numpy as jnp
from jax import lax
from jax.experimental import pallas as pl
from jax.experimental.pallas import tpu as pltpu
from jax.sharding import PartitionSpec as P

AXES = ("gx", "gy", "gz")
MESH = pl.DeviceIdType.MESH
F32, BF16, I32 = jnp.float32, jnp.bfloat16, jnp.int32
CHUNKS = 2
FRONT = 1280
LATE = 150


def split2(v):
    hi = v.astype(BF16)
    lo = (v - hi.astype(F32)).astype(BF16)
    return hi, lo


def split3(v):
    hi = v.astype(BF16)
    rest = v - hi.astype(F32)
    mid = rest.astype(BF16)
    lo = (rest - mid.astype(F32)).astype(BF16)
    return hi, mid, lo


def dot(a, b):
    return jnp.dot(a, b, preferred_element_type=F32)


def kernel(
    sizes,
    measures, index_in, keys_in,
    arrived, small,
    values, index, keys, acc, tally, halves, near, outgoing, fsend, frecv, fown, fline,
    crow, cline, crelay, call,
    load_sems, own_sems, near_send, near_recv, cz_send, cz_recv, cp_send, cp_recv, fp_send, fp_recv, fz_send, fz_recv, b_send, b_recv,
):
    nx, ny, nz = sizes
    plane, devices = nx * ny, nx * ny * nz
    rows = measures.shape[0]
    bounds = ((0, FRONT), (FRONT, rows))
    span = 2 * devices
    x, y, z = (lax.axis_index(a) for a in AXES)
    q = x * ny + y
    me = q * nz + z

    def outward(n):
        return sorted(range(n), key=lambda k: -min(k, n - k))

    def moved(base, k, n):
        return lax.rem(base + k, n) if k else base

    lines = [(k, moved(z, k, nz)) for k in outward(nz) if k]
    across = sorted(
        ((i, j) for i in range(nx) for j in range(ny) if i or j),
        key=lambda t: -(min(t[0], nx - t[0]) + min(t[1], ny - t[1]) / 2),
    )
    xs = [moved(x, k, nx) for k in range(nx)]
    ys = [moved(y, k, ny) for k in range(ny)]
    peers = [(xs[i], ys[j]) for i, j in across]

    barrier = pltpu.get_barrier_semaphore()
    greeted = [(min(i, nx - i) + min(j, ny - j) / 2, (px, py, z)) for (i, j), (px, py) in zip(across, peers)]
    greeted += [(min(k, nz - k), (x, y, tz)) for k, tz in lines]
    for _, place in sorted(greeted, key=lambda t: -t[0]):
        pl.semaphore_signal(barrier, inc=1, device_id=place, device_id_type=MESH)

    loads = [
        pltpu.make_async_copy(
            measures.at[pl.ds(low, high - low)], values.at[pl.ds(low, high - low)], load_sems.at[c]
        )
        for c, (low, high) in enumerate(bounds)
    ]
    inputs = [
        pltpu.make_async_copy(src, dst, load_sems.at[CHUNKS + i])
        for i, (src, dst) in enumerate(((index_in, index), (keys_in, keys)))
    ]
    for load in inputs + loads:
        load.start()

    for load in inputs:
        load.wait()
    count = jnp.max(index[...], axis=1, keepdims=True) + 1
    lane = lax.broadcasted_iota(I32, (1, 128), 1)
    mine = jnp.where(lane == me % 128, count, 0)
    crow[0] = mine
    cline[z] = mine


    def accumulate(c):
        low, high = bounds[c]
        step = high - low
        labels = lax.broadcasted_iota(I32, (span, step), 0)
        ones = jnp.ones((step, 128), BF16)
        loads[c].wait()
        hits = jnp.where(labels == index[0:1, low:high], 1.0, 0.0).astype(BF16)
        hi, lo = split2(values[pl.ds(low, step)])
        part = dot(hits, hi) + dot(hits, lo)
        seen = dot(hits, ones)
        if c == 0:
            acc[...] = part
            tally[...] = seen
        else:
            acc[...] += part
            tally[...] += seen

    for c in range(CHUNKS // 2):
        accumulate(c)
    pl.semaphore_wait(barrier, nz - 1 + plane - 1)

    for _, tz in lines:
        pltpu.make_async_remote_copy(
            crow.at[0], cline.at[z], cz_send, cz_recv, device_id=(x, y, tz), device_id_type=MESH
        ).start()
    for c in range(CHUNKS // 2, CHUNKS):
        accumulate(c)

    def drain(ref, n, sem):
        pltpu.make_async_copy(ref.at[pl.ds(0, n)], ref.at[pl.ds(0, n)], sem).wait()

    for half in range(2):
        for level in range(2):
            part = acc[pl.ds(level * devices, devices), pl.ds(half * 128, 128)]
            halves[half, level, pl.ds(0, devices), :] = part
            halves[half, level, pl.ds(devices, devices), :] = part
    for half, tz in ((0, moved(z, 1, nz)), (1, moved(z, nz - 1, nz))):
        for level in range(2):
            pltpu.make_async_remote_copy(
                halves.at[half, level, pl.ds(0, devices)], near.at[half, level, pl.ds(0, devices)],
                near_send, near_recv, device_id=(x, y, tz), device_id_type=MESH,
            ).start()
    seen = tally[...].T[0:1]
    named = keys[...].astype(F32) + 1.0
    fown[0] = jnp.concatenate(
        [row[:, level * devices : (level + 1) * devices] for row in (seen, named) for level in range(2)], axis=0
    )
    fline[z] = fown[0]
    for _, tz in lines:
        pltpu.make_async_remote_copy(
            fown.at[0], fline.at[z], fz_send, fz_recv, device_id=(x, y, tz), device_id_type=MESH
        ).start()
    drain(cline, nz - 1, cz_recv)
    relayed = cline[0]
    for k in range(1, nz):
        relayed = relayed + cline[k]
    crelay[0] = relayed
    call[q] = relayed

    for px, py in peers:
        pltpu.make_async_remote_copy(
            crelay.at[0], call.at[q], cp_send, cp_recv, device_id=(px, py, z), device_id_type=MESH
        ).start()

    pltpu.make_async_copy(acc, acc, near_recv).wait()
    for half in range(2):
        for level in range(2):
            near[half, level, pl.ds(devices, devices), :] = near[half, level, pl.ds(0, devices), :]
    drain(call, plane - 1, cp_recv)
    low = jnp.sum(call[pl.ds(0, plane // 2)], axis=0)
    high = jnp.sum(call[pl.ds(plane // 2, plane // 2)], axis=0)
    counts = jnp.concatenate([low, high], axis=1)
    lanes = lax.broadcasted_iota(I32, (1, devices), 1)

    def start_of(device):
        return devices - lax.rem(jnp.sum(jnp.where(lanes < device, counts, 0)), devices)

    start = start_of(me)
    for level in range(2):
        outgoing[0, pl.ds(level, devices, stride=4), :] = halves[1, level, pl.ds(start, devices), :]
        outgoing[1, pl.ds(level, devices, stride=4), :] = halves[0, level, pl.ds(start, devices), :]
    for half, other in ((0, moved(z, nz - 1, nz)), (1, moved(z, 1, nz))):
        first = start_of(q * nz + other)
        for level in range(2):
            outgoing[half, pl.ds(2 + level, devices, stride=4), :] = near[half, level, pl.ds(first, devices), :]

    reach = nz // 2

    def hops(offset):
        i, j, side, k = offset
        return 2 * (min(i, nx - i) + min(j, ny - j) / 2 + (j % 2) * 0.1) + k

    order = sorted(
        (
            (i, j, side, k)
            for i in range(nx) for j in range(ny) for side in range(2) for k in range(reach) if i or j or k
        ),
        key=lambda t: (-hops(t), t),
    )
    zs = [moved(z, k, nz) for k in range(nz)]

    def send_blocks(offsets):
        for i, j, side, k in offsets:
            px, py, tz = xs[i], ys[j], zs[(nz - k) % nz if side else k]
            target = (px * ny + py) * nz + tz
            pltpu.make_async_remote_copy(
                outgoing.at[side, pl.ds(4 * target, 4)],
                arrived.at[(side * plane + q) * reach + k],
                b_send, b_recv, device_id=(px, py, tz), device_id_type=MESH,
            ).start()

    send_blocks(order[:LATE])
    drain(fline, nz - 1, fz_recv)
    group = lax.broadcasted_iota(I32, (plane, devices), 1)
    target = lax.broadcasted_iota(I32, (plane, devices), 0) * nz + z
    picked = jnp.concatenate(
        [
            jnp.where(group == lax.rem(target + start_of(q * nz + k), devices), 1.0, 0.0).astype(BF16)
            for k in range(nz)
        ],
        axis=0,
    )
    table = jnp.concatenate(
        [fline[k] for k in range(nz)] + [jnp.zeros((128 - 4 * nz, devices), F32)], axis=0
    )
    sent = sum(
        lax.dot_general(picked, part, (((1,), (1,)), ((), ())), preferred_element_type=F32)
        for part in split3(table)
    )
    flane = lax.broadcasted_iota(I32, (devices, 128), 1)
    frow = lax.broadcasted_iota(I32, (devices, 128), 0)
    sent = jnp.where(lax.div(flane, 4) == lax.div(frow, plane), sent, 0.0)
    fsend[...] = jnp.sum(sent.reshape(nz, plane, 128), axis=0).reshape(plane, 1, 128)
    for px, py in peers:
        pltpu.make_async_remote_copy(
            fsend.at[px * ny + py], frecv.at[q], fp_send, fp_recv, device_id=(px, py, z), device_id_type=MESH
        ).start()
    send_blocks(order[LATE:])
    owns = [
        pltpu.make_async_copy(
            outgoing.at[side, pl.ds(4 * me, 4)], arrived.at[(side * plane + q) * reach], own_sems.at[side]
        )
        for side in range(2)
    ]
    for own in owns:
        own.start()

    before = lax.broadcasted_iota(I32, (devices, devices), 0) < lax.broadcasted_iota(I32, (devices, devices), 1)
    before = jnp.where(before, 1.0, 0.0).astype(BF16)
    tops = jnp.broadcast_to((counts // 8).astype(F32).astype(BF16), (8, devices))
    rests = jnp.broadcast_to((counts % 8).astype(F32).astype(BF16), (8, devices))
    offsets = (8.0 * dot(tops, before) + dot(rests, before))[0:1].astype(I32)
    places = []
    for level in range(2):
        position = level * devices + (me - offsets) % devices
        place = (offsets + position) // devices
        places.append(jnp.where(position < counts, place, -1))
    place = jnp.concatenate(places, axis=1)
    picks = jnp.where(lax.broadcasted_iota(I32, (span, span), 0) == place, 1.0, 0.0).astype(BF16)

    frecv[q] = fsend[q]
    drain(frecv, plane - 1, fp_recv)
    wide = jnp.broadcast_to(frecv[...], (plane, nz, 128)).reshape(devices, 128)
    fit = lax.div(flane, 4) == lax.rem(frow, nz)
    chosen = jnp.concatenate(
        [jnp.where(fit & (lax.rem(flane, 2) == level), wide, 0.0) for level in range(2)], axis=0
    )
    hi, mid, lo = split3(chosen)
    found = ((dot(picks, hi) + dot(picks, mid)) + dot(picks, lo)).T
    is_key = lax.rem(lax.broadcasted_iota(I32, (128, span), 0), 4) >= 2
    small[0:1] = jnp.sum(jnp.where(is_key, 0.0, found), axis=0, keepdims=True).astype(I32)
    small[1:2] = jnp.sum(jnp.where(is_key, found, 0.0), axis=0, keepdims=True).astype(I32) - 1
    level_row = lax.broadcasted_iota(I32, (8, devices), 0)
    natural = jnp.where(level_row == 0, place[:, :devices], place[:, devices:]).astype(F32) + 1.0
    hi, lo = split2(natural)
    slot = lax.broadcasted_iota(I32, (devices, devices), 1)
    holder = lax.div(lax.rem(slot, devices // 2), reach)
    shift = lax.rem(slot, reach)
    direct = slot < devices // 2
    for row, step_z in (
        (2, jnp.where(direct, nz + shift, nz - shift - 1)),
        (3, jnp.where(direct, nz - shift, nz + shift + 1)),
    ):
        source = holder * nz + lax.rem(z + step_z, nz)
        match = lax.broadcasted_iota(I32, (devices, devices), 0) == source
        match = jnp.where(match, 1.0, 0.0).astype(BF16)
        ordered = (dot(hi, match) + dot(lo, match)).astype(I32) - 1
        small[row : row + 1] = jnp.concatenate([ordered[0:1], ordered[1:2]], axis=1)
    small[4:5] = jnp.broadcast_to(jnp.sum(counts, axis=1, keepdims=True), (1, span))
    for own in owns:
        own.wait()
    drain(arrived, devices - 2, b_recv)
    drain(cline, nz - 1, cz_send)
    drain(call, plane - 1, cp_send)
    drain(fsend, plane - 1, fp_send)
    drain(fline, nz - 1, fz_send)
    drain(arrived, devices - 2, b_send)
    pltpu.make_async_copy(acc, acc, near_send).wait()


def put(arrived, small, out_sums, out_rows, out_keys, out_total):
    span = out_sums.shape[0]
    senders = span // 2
    slots = senders // 2
    out_rows[...] = small[0:1]
    out_keys[...] = small[1:2]
    out_total[...] = small[4:5, 0:1]
    labels = lax.broadcasted_iota(I32, (span, senders), 0)
    sides = []
    for half in range(2):
        direct, relayed = (4 * slots, 2) if half == 0 else (0, 4 * slots + 2)
        total = None
        for level in range(2):
            block = jnp.concatenate(
                [arrived[pl.ds(base + level, slots, stride=4), :] for base in (direct, relayed)], axis=0
            )
            places = small[2 + half : 3 + half, level * senders : (level + 1) * senders]
            picks = jnp.where(labels == places, 1.0, 0.0).astype(BF16)
            part = dot(picks, jnp.concatenate(split2(block), axis=1))
            total = part if total is None else total + part
        sides.append(total[:, :128] + total[:, 128:])
    out_sums[...] = jnp.concatenate(sides, axis=1)


def solution(mesh):
    sizes = tuple(mesh.shape[a] for a in AXES)
    nx, ny, nz = sizes
    plane, devices = nx * ny, nx * ny * nz
    vmem = pl.BlockSpec(memory_space=pltpu.VMEM)

    def shards(measures, group_index, distinct_keys, group_counts):
        rows, width = measures.shape
        span = distinct_keys.shape[1]
        hbm = pl.BlockSpec(memory_space=pl.ANY)
        arrived, small = pl.pallas_call(
            functools.partial(kernel, sizes),
            out_shape=(
                jax.ShapeDtypeStruct((devices, 4, 128), F32),
                jax.ShapeDtypeStruct((8, span), I32),
            ),
            in_specs=[hbm] * 3,
            out_specs=(pl.BlockSpec(memory_space=pl.ANY), vmem),
            scratch_shapes=[
                pltpu.VMEM((rows, width), F32),
                pltpu.VMEM((1, rows), I32),
                pltpu.VMEM((1, span), I32),
                pltpu.VMEM((span, width), F32),
                pltpu.VMEM((span, 128), F32),
                pltpu.VMEM((2, 2, span, 128), F32),
                pltpu.VMEM((2, 2, span, 128), F32),
                pltpu.VMEM((2, 4 * devices, 128), F32),
                pltpu.VMEM((plane, 1, 128), F32),
                pltpu.VMEM((plane, 1, 128), F32),
                pltpu.VMEM((1, 4, devices), F32),
                pltpu.VMEM((nz, 4, devices), F32),
                pltpu.VMEM((1, 1, 128), I32),
                pltpu.VMEM((nz, 1, 128), I32),
                pltpu.VMEM((1, 1, 128), I32),
                pltpu.VMEM((plane, 1, 128), I32),
                pltpu.SemaphoreType.DMA((CHUNKS + 2,)),
                pltpu.SemaphoreType.DMA((2,)),
            ]
            + [pltpu.SemaphoreType.DMA(())] * 12,
            compiler_params=pltpu.CompilerParams(
                collective_id=0, has_side_effects=True, vmem_limit_bytes=32 << 20
            ),
            name="exchange",
        )(*(
            pltpu.with_memory_space_constraint(a, pltpu.MemorySpace.HBM)
            for a in (measures, group_index.reshape(1, rows), distinct_keys)
        ))
        sums, tallies, keys, total = pl.pallas_call(
            put,
            out_shape=(
                jax.ShapeDtypeStruct((span, width), F32),
                jax.ShapeDtypeStruct((1, span), I32),
                jax.ShapeDtypeStruct((1, span), I32),
                jax.ShapeDtypeStruct((1, 1), I32),
            ),
            in_specs=[vmem] * 2,
            out_specs=(vmem,) * 4,
            compiler_params=pltpu.CompilerParams(vmem_limit_bytes=24 << 20),
            name="put",
        )(arrived.reshape(4 * devices, 128), small)
        return sums, tallies.reshape(span), keys.reshape(span), total.reshape(())

    return jax.shard_map(
        shards,
        mesh=mesh,
        in_specs=(P(AXES, None), P(AXES), P(AXES, None), P(AXES)),
        out_specs=(P(AXES, None), P(AXES), P(AXES), P()),
        check_vma=False,
    )
```
